32 devices in a mesh: space: 8 (over y, x, core), tm: 4 (over z).
Axes of the slice: x: 2, y: 2, z: 4, core: 2. Of those that a mesh axis runs over, the one named last changes fastest.
Arguments:
- tensor: float32 [512, 64, 512], P('space', None, 'tm'), may hold values from -6 to 6
- species_factor: float32 [64, 256], replicated, may hold values from -6 to 6
- time_factor: float32 [512, 256], P('tm'), may hold values from -6 to 6
Outputs:
- space_out: float32 [512, 256], P('space')
- species_out: float32 [64, 256], replicated
- time_out: float32 [512, 256], P('tm')
The draws below stay inside these ranges and needn't reach their ends.
All inputs are finite; a program needn't handle non-finite values.
Results may differ from the reference program's by a relative error of at most 0.0001.
Values sent between devices are 32-bit elements; how exact they have to be, the bound alone decides.
No kernel may reach another device: no remote copies, remote signals or barrier semaphores. Data moves between devices by JAX's collectives and lax.ppermute only.
A program may use at most 64 MiB of HBM per device.

```python
import jax
import jax.numpy as jnp
from jax import lax

R = 256
P_SIZE = 64
SPD = 64
NS = 512
NT = 512


def shard_levels(stream_key, shape, shards, smallest, largest):
    def one(dim, blocks):
        draws = jax.random.uniform(jax.random.fold_in(jax.random.fold_in(stream_key, 6), dim), (blocks,), jnp.float32, smallest / len(shards), largest / len(shards))
        return jnp.repeat(jnp.exp(draws), shape[dim] // blocks).reshape((-1,) + (1,) * (len(shape) - dim - 1))

    level = one(*shards[0])
    for cut in shards[1:]:
        level = level * one(*cut)
    return level


def normal_values(rng, shape, width, bound, pieces=(), kind=jnp.bfloat16):
    drawn = jax.random.normal(rng, shape, jnp.float32) * width
    if len(pieces) > 0:
        drawn = shard_levels(rng, shape, pieces, -0.22, 0.18) * drawn
    return jnp.clip(drawn, min=-bound, max=bound).astype(kind)


def setup_inputs(seed: int = 0) -> dict:
    seeds = jax.random.split(jax.random.key(seed), 4)
    return {
        "tensor": normal_values(seeds[0], (NS, P_SIZE, NT), 1.0, 6.0, ((0, 8), (2, 4)), jnp.float32),
        "species_factor": normal_values(seeds[1], (P_SIZE, R), 1.0, 6.0, (), jnp.float32),
        "time_factor": normal_values(seeds[2], (NT, R), 1.0, 6.0, ((0, 4),), jnp.float32),
    }


ridge_share = 0.1
epsilon = 1e-06

def cross_gram(factor):
    return jnp.dot(factor.T.astype(jnp.float32), factor.astype(jnp.float32), precision=lax.Precision.HIGHEST, preferred_element_type=jnp.float32)

def solve_rows(partial_value, matrix):
    rank_count = matrix.shape[0]
    regular = matrix + ridge_share * jnp.trace(matrix) / rank_count * jnp.eye(rank_count, dtype=matrix.dtype)
    lower_factor = jnp.linalg.cholesky(regular)
    return jax.scipy.linalg.cho_solve((lower_factor, True), partial_value.T).T

def unit_columns(factor):
    return factor * lax.rsqrt(lax.optimization_barrier(jnp.mean(factor * factor, axis=0)) + epsilon)

def reference(tensor, species_factor, time_factor):
    highest = lax.Precision.HIGHEST
    rank_count = species_factor.shape[1]
    total_space = tensor.shape[0]
    steps_all = tensor.shape[2]
    c_gram = cross_gram(time_factor)
    b_gram = cross_gram(species_factor)
    blocks = tensor.reshape(total_space // SPD, SPD, P_SIZE, steps_all)

    def space_products(tensor_block):
        space_side = jnp.dot(tensor_block.reshape(SPD * P_SIZE, steps_all).astype(jnp.float32), time_factor.astype(jnp.float32), precision=highest, preferred_element_type=jnp.float32).reshape(SPD, P_SIZE, rank_count)
        return jnp.einsum('spr,pr->sr', space_side, species_factor, precision=highest)
    m_a = lax.map(space_products, blocks).reshape(total_space, rank_count)
    space_out = unit_columns(solve_rows(m_a, b_gram * c_gram))
    a_gram = cross_gram(space_out)
    factor_blocks = space_out.reshape(total_space // SPD, SPD, rank_count)

    def accumulate(running, paired):
        tensor_block, factor = paired
        piece = lax.dot_general(tensor_block.reshape(SPD, P_SIZE * steps_all).astype(jnp.float32), factor.astype(jnp.float32), (((0,), (0,)), ((), ())), precision=highest, preferred_element_type=jnp.float32)
        return (running + piece, None)
    time_side, _ = lax.scan(accumulate, jnp.zeros((P_SIZE * steps_all, rank_count), jnp.float32), (blocks, factor_blocks))
    time_side = time_side.reshape(P_SIZE, steps_all, rank_count)
    m_b = jnp.einsum('ptr,tr->pr', time_side, time_factor, precision=highest)
    species_out = unit_columns(solve_rows(m_b, a_gram * c_gram))
    m_c = jnp.einsum('ptr,pr->tr', time_side, species_out, precision=highest)
    time_out = unit_columns(solve_rows(m_c, a_gram * cross_gram(species_out)))
    return (space_out, species_out, time_out)
```

```python
import jax
import jax.numpy as jnp
from jax import lax
from jax.experimental import pallas as pl
from jax.experimental.pallas import tpu as pltpu
from jax.sharding import PartitionSpec as P

ridge_share = 0.1
epsilon = 1e-06
contraction_bound = 1e-3
highest = lax.Precision.HIGHEST
f32 = jnp.float32
bf16 = jnp.bfloat16

vmem = pl.BlockSpec(memory_space=pltpu.VMEM)
smem = pl.BlockSpec(memory_space=pltpu.SMEM)


def dot(a, b, dims=((1,), (0,))):
    return lax.dot_general(a, b, (dims, ((), ())), precision=highest, preferred_element_type=f32)


def dot_fast(a, b, dims=((1,), (0,))):
    return lax.dot_general(a, b, (dims, ((), ())), preferred_element_type=f32)


def gram(factor):
    return dot(factor, factor, ((0,), (0,)))


def split(x):
    high = x.astype(bf16)
    return high, (x - high.astype(f32)).astype(bf16)


def tree_sum(values):
    values = list(values)
    while len(values) > 1:
        values = [a + b for a, b in zip(values[0::2], values[1::2])]
    return values[0]


def eye_mask(n):
    return lax.broadcasted_iota(jnp.int32, (n, n), 0) == lax.broadcasted_iota(jnp.int32, (n, n), 1)


def regularized(matrix):
    n = matrix.shape[0]
    eye = eye_mask(n)
    diagonal = jnp.where(eye, matrix, 0.0)
    ridge = ridge_share * jnp.sum(diagonal) / n
    return matrix + jnp.where(eye, ridge, 0.0)


def invert(matrix, x_ref, work_ref):
    n = matrix.shape[0]
    eye = eye_mask(n)
    diagonal = jnp.where(eye, matrix, 0.0)
    by_column = lax.rsqrt(jnp.sum(diagonal, axis=0, keepdims=True))
    by_row = lax.rsqrt(jnp.sum(diagonal, axis=1, keepdims=True))
    e1 = jnp.where(eye, 0.0, -(matrix * by_column) * by_row)
    e1_half = e1.astype(bf16)
    e2 = dot_fast(e1_half, e1_half)
    e2_half = e2.astype(bf16)
    e4 = dot_fast(e2_half, e2_half)
    e4_half = e4.astype(bf16)
    part = e1 + e2 + dot_fast(e1_half, e2_half)
    part = part + e4 + dot_fast(part.astype(bf16), e4_half)
    left = jnp.sum(e4 * e4)
    x_ref[...] = (part + jnp.where(eye, 1.0, 0.0)) * by_column * by_row

    @pl.when(jnp.logical_not(left < contraction_bound))
    def _():
        work_ref[...] = jnp.where(eye, 1.0, 0.0) - e1
        lane = lax.broadcasted_iota(jnp.int32, (n, n), 1)
        sublane = lax.broadcasted_iota(jnp.int32, (n, n), 0)
        lane_row = lax.broadcasted_iota(jnp.int32, (1, n), 1)

        def step(k, carry):
            work = work_ref[...]
            row = work_ref[pl.ds(k, 1), :]
            pivot = jnp.sum(jnp.where(lane_row == k, row, 0.0), axis=1, keepdims=True)
            column = jnp.sum(jnp.where(lane == k, work, 0.0), axis=1, keepdims=True)
            inverse = 1.0 / pivot
            new_row = jnp.where(lane_row == k, inverse, row * inverse)
            others = jnp.where(lane == k, 0.0, work) - column * new_row
            work_ref[...] = jnp.where(sublane == k, new_row, others)
            return carry

        lax.fori_loop(0, n, step, 0)
        x_ref[...] = work_ref[...] * by_column * by_row


def solve(right, matrix, inverse):
    first = dot(right, inverse)
    return first + dot(right - dot(first, matrix), inverse)


def space_kernel(tensor_ref, time_ref, species_ref, m_a_ref, side_ref):
    rows, species_count, steps = tensor_ref.shape
    high, low = split(tensor_ref[...].reshape(rows * species_count, steps))
    both = jnp.concatenate([high, low], axis=1)
    time_high, time_low = split(time_ref[...])
    side = dot_fast(both, jnp.concatenate([time_high, time_low], axis=0))
    side = side + dot_fast(both, jnp.concatenate([time_low, time_high], axis=0))
    side = side.reshape(rows, species_count, side.shape[1])
    side_ref[...] = side
    m_a_ref[...] = jnp.sum(side * species_ref[...][None], axis=1)


def first_inverse_kernel(place_ref, species_ref, own_ref, *refs):
    *halves, c_gram_ref, matrix_ref, inverse_ref, factor_ref, work_ref = refs
    block, core = place_ref[0], place_ref[1]
    rows = own_ref.shape[0]
    half = halves[0].shape[0] if halves else 0
    factor_ref[pl.ds(pl.multiple_of(block * rows, rows), rows), :] = own_ref[...]
    count = len(halves) // 2
    for j in range(1, count + 1):
        other = jnp.bitwise_xor(block, j) * rows
        factor_ref[pl.ds(pl.multiple_of(other + core * half, half), half), :] = halves[j - 1][...]
        partner = other + (1 - core) * half
        factor_ref[pl.ds(pl.multiple_of(partner, half), half), :] = halves[count + j - 1][...]
    c_gram = gram(factor_ref[...])
    c_gram_ref[...] = c_gram
    matrix = regularized(gram(species_ref[...]) * c_gram)
    matrix_ref[...] = matrix
    invert(matrix, inverse_ref, work_ref)


def space_solve_kernel(place_ref, matrix_ref, inverse_ref, side_ref, *refs):
    *parts, raw_ref, keep_ref, send_ref, product_ref = refs
    core = place_ref[1]
    m_a = tree_sum([part[...] for part in parts])
    raw = solve(m_a, matrix_ref[...], inverse_ref[...])
    raw_ref[...] = raw
    rows = side_ref.shape[0]
    total = jnp.zeros(product_ref.shape, f32)
    for s in range(rows):
        total = total + side_ref[s] * raw_ref[pl.ds(s, 1), :]
    product_ref[...] = total
    half = keep_ref.shape[0]
    keep_ref[...] = product_ref[pl.ds(pl.multiple_of(core * half, half), half), :]
    send_ref[...] = product_ref[pl.ds(pl.multiple_of((1 - core) * half, half), half), :]


def second_inverse_kernel(place_ref, c_gram_ref, *refs):
    (*blocks, a_gram_ref, matrix_ref, inverse_ref, scale_ref, raw_scaled_ref, factor_ref, work_ref) = refs
    place = place_ref[2]
    rows = blocks[0].shape[0]
    for j, block in enumerate(blocks):
        at = jnp.bitwise_xor(place, j) * rows
        factor_ref[pl.ds(pl.multiple_of(at, rows), rows), :] = block[...]
    raw_gram = gram(factor_ref[...])
    n = raw_gram.shape[0]
    eye = eye_mask(n)
    diagonal = jnp.where(eye, raw_gram, 0.0)
    total_rows = factor_ref.shape[0]
    by_column = lax.rsqrt(jnp.sum(diagonal, axis=0, keepdims=True) / total_rows + epsilon)
    by_row = lax.rsqrt(jnp.sum(diagonal, axis=1, keepdims=True) / total_rows + epsilon)
    scale_ref[...] = jnp.broadcast_to(by_column, scale_ref.shape)
    raw_scaled_ref[...] = blocks[0][...] * by_column
    a_gram = raw_gram * by_column * by_row
    a_gram_ref[...] = a_gram
    matrix = regularized(a_gram * c_gram_ref[...])
    matrix_ref[...] = matrix
    invert(matrix, inverse_ref, work_ref)


def species_kernel(place_ref, mine_ref, partner_ref, scale_ref, matrix_ref, inverse_ref, space_ref, tensor_ref,
                   species_ref, keep_ref, send_ref, m_b_ref, product_ref):
    core = place_ref[1]
    half = mine_ref.shape[0]
    m_b_ref[pl.ds(pl.multiple_of(core * half, half), half), :] = mine_ref[...]
    m_b_ref[pl.ds(pl.multiple_of((1 - core) * half, half), half), :] = partner_ref[...]
    m_b = m_b_ref[...] * scale_ref[0:1, :]
    raw = solve(m_b, matrix_ref[...], inverse_ref[...])
    species = raw * lax.rsqrt(jnp.mean(raw * raw, axis=0, keepdims=True) + epsilon)
    species_ref[...] = species
    rows, species_count, steps = tensor_ref.shape
    chunk = 8
    total = jnp.zeros(product_ref.shape, f32)
    for start in range(0, rows, chunk):
        weights = species[None] * space_ref[start:start + chunk, :][:, None, :]
        weights = weights.reshape(chunk * species_count, species.shape[1])
        weights_high, weights_low = split(weights)
        high, low = split(tensor_ref[start:start + chunk].reshape(chunk * species_count, steps))
        rows_first = ((0,), (0,))
        total = total + dot_fast(high, weights_high, rows_first)
        total = total + (dot_fast(high, weights_low, rows_first) + dot_fast(low, weights_high, rows_first))
    product_ref[...] = total
    half = keep_ref.shape[0]
    keep_ref[...] = product_ref[pl.ds(pl.multiple_of(core * half, half), half), :]
    send_ref[...] = product_ref[pl.ds(pl.multiple_of((1 - core) * half, half), half), :]


def third_inverse_kernel(a_gram_ref, species_ref, matrix_ref, inverse_ref, work_ref):
    matrix = regularized(a_gram_ref[...] * gram(species_ref[...]))
    matrix_ref[...] = matrix
    invert(matrix, inverse_ref, work_ref)


def time_solve_kernel(matrix_ref, inverse_ref, *refs):
    *parts, out_ref = refs
    m_c = tree_sum([part[...] for part in parts])
    raw = solve(m_c, matrix_ref[...], inverse_ref[...])
    rows = raw.shape[0]
    out_ref[:rows, :] = raw
    squares = jnp.sum(raw * raw, axis=0, keepdims=True)
    out_ref[rows:, :] = jnp.broadcast_to(squares, (out_ref.shape[0] - rows, raw.shape[1]))


def time_scale_kernel(total_steps, place_ref, mine_ref, partner_ref, *refs):
    *parts, out_ref = refs
    core = place_ref[1]
    half = out_ref.shape[0] // 2
    squares = tree_sum([part[0:1, :] for part in parts])
    scale = lax.rsqrt(squares / total_steps + epsilon)
    out_ref[pl.ds(pl.multiple_of(core * half, half), half), :] = mine_ref[:half, :] * scale
    out_ref[pl.ds(pl.multiple_of((1 - core) * half, half), half), :] = partner_ref[:half, :] * scale


def exchange(value, axis, step, count):
    return lax.ppermute(value, axis, [(i, i ^ step) for i in range(count)])


def on_device(tensor, species_factor, time_factor):
    row_count, species_count, step_count = tensor.shape
    rank = species_factor.shape[1]
    devices = lax.axis_size("space")
    blocks = lax.axis_size("tm")
    total_rows = row_count * devices
    total_steps = step_count * blocks
    place_space = lax.axis_index("space")
    place_time = lax.axis_index("tm")
    core = place_space % 2
    place = jnp.stack([place_time, core, place_space]).astype(jnp.int32)

    def shape(*dims):
        return jax.ShapeDtypeStruct(dims, f32)

    square = shape(rank, rank)
    square_scratch = pltpu.VMEM((rank, rank), f32)

    def over_time(value):
        return [value] + [exchange(value, "tm", j, blocks) for j in range(1, blocks)]

    def over_chips(value):
        return [value] + [exchange(value, "space", 2 * j, devices) for j in range(1, devices // 2)]

    def to_partner(value):
        return exchange(value, "space", 1, devices)

    half_steps = step_count // 2
    own_half = lax.dynamic_slice_in_dim(time_factor, core * half_steps, half_steps)
    halves = over_time(own_half)[1:]
    partner_halves = [to_partner(half) for half in halves]

    slab = 8
    m_a, side = pl.pallas_call(
        space_kernel,
        grid=(row_count // slab,),
        in_specs=[
            pl.BlockSpec((slab, species_count, step_count), lambda i: (i, 0, 0)),
            pl.BlockSpec((step_count, rank), lambda i: (0, 0)),
            pl.BlockSpec((species_count, rank), lambda i: (0, 0)),
        ],
        out_specs=[
            pl.BlockSpec((slab, rank), lambda i: (i, 0)),
            pl.BlockSpec((slab, species_count, rank), lambda i: (i, 0, 0)),
        ],
        out_shape=[shape(row_count, rank), shape(row_count, species_count, rank)],
        name="space_products",
    )(tensor, time_factor, species_factor)
    m_a_parts = over_time(m_a)

    c_gram, matrix, inverse = pl.pallas_call(
        first_inverse_kernel,
        in_specs=[smem] + [vmem] * (2 + 2 * len(halves)),
        out_specs=[vmem] * 3,
        out_shape=[square] * 3,
        scratch_shapes=[pltpu.VMEM((total_steps, rank), f32), square_scratch],
        name="first_inverse",
    )(place, species_factor, time_factor, *halves, *partner_halves)

    half_species = species_count // 2
    raw, m_b_keep, m_b_send = pl.pallas_call(
        space_solve_kernel,
        in_specs=[smem] + [vmem] * (3 + len(m_a_parts)),
        out_specs=[vmem] * 3,
        out_shape=[shape(row_count, rank), shape(half_species, rank), shape(half_species, rank)],
        scratch_shapes=[pltpu.VMEM((species_count, rank), f32)],
        name="space_solve",
    )(place, matrix, inverse, side, *m_a_parts)

    m_b = m_b_keep + to_partner(m_b_send)
    raw_chips = over_chips(raw)
    m_b = tree_sum(over_time(m_b))
    raw_all = []
    for block in raw_chips:
        raw_all += [block, to_partner(block)]
    m_b = tree_sum(over_chips(m_b))
    m_b_partner = to_partner(m_b)

    a_gram, matrix, inverse, scale, space_out = pl.pallas_call(
        second_inverse_kernel,
        in_specs=[smem] + [vmem] * (1 + len(raw_all)),
        out_specs=[vmem] * 5,
        out_shape=[square] * 3 + [shape(8, rank), shape(row_count, rank)],
        scratch_shapes=[pltpu.VMEM((total_rows, rank), f32), square_scratch],
        name="second_inverse",
    )(place, c_gram, *raw_all)

    species_out, m_c_keep, m_c_send = pl.pallas_call(
        species_kernel,
        in_specs=[smem] + [vmem] * 7,
        out_specs=[vmem] * 3,
        out_shape=[shape(species_count, rank), shape(half_steps, rank), shape(half_steps, rank)],
        scratch_shapes=[pltpu.VMEM((species_count, rank), f32), pltpu.VMEM((step_count, rank), f32)],
        name="species_solve",
    )(place, m_b, m_b_partner, scale, matrix, inverse, space_out, tensor)

    m_c = m_c_keep + to_partner(m_c_send)
    m_c_parts = over_chips(m_c)

    matrix, inverse = pl.pallas_call(
        third_inverse_kernel,
        in_specs=[vmem] * 2,
        out_specs=[vmem] * 2,
        out_shape=[square] * 2,
        scratch_shapes=[square_scratch],
        name="third_inverse",
    )(a_gram, species_out)

    raw_time = pl.pallas_call(
        time_solve_kernel,
        in_specs=[vmem] * (2 + len(m_c_parts)),
        out_specs=vmem,
        out_shape=shape(half_steps + 8, rank),
        name="time_solve",
    )(matrix, inverse, *m_c_parts)

    partner_time = to_partner(raw_time)
    squares = over_time(raw_time[half_steps:] + partner_time[half_steps:])

    time_out = pl.pallas_call(
        lambda *refs: time_scale_kernel(total_steps, *refs),
        in_specs=[smem] + [vmem] * (2 + len(squares)),
        out_specs=vmem,
        out_shape=shape(step_count, rank),
        name="time_scale",
    )(place, raw_time, partner_time, *squares)
    return (space_out, species_out, time_out)


def solution(mesh):
    placed = (P("space", None, "tm"), P(), P("tm", None))
    return jax.shard_map(
        on_device,
        mesh=mesh,
        in_specs=placed,
        out_specs=(P("space", None), P(), P("tm", None)),
        check_vma=False,
    )
```

```python
import jax
import jax.numpy as jnp
from jax import lax
from jax.experimental import pallas as pl
from jax.experimental.pallas import tpu as pltpu
from jax.sharding import PartitionSpec as P

ridge_share = 0.1
epsilon = 1e-06
contraction_bound = 1e-3
highest = lax.Precision.HIGHEST
f32 = jnp.float32
bf16 = jnp.bfloat16

vmem = pl.BlockSpec(memory_space=pltpu.VMEM)
flops_per_micro = 1e9
vmem_limit = 24 * 1024 * 1024


def dot(a, b, dims=((1,), (0,))):
    return lax.dot_general(a, b, (dims, ((), ())), precision=highest, preferred_element_type=f32)


def dot_fast(a, b, dims=((1,), (0,))):
    return lax.dot_general(a, b, (dims, ((), ())), preferred_element_type=f32)


def gram(factor):
    return dot(factor, factor, ((0,), (0,)))


def split(x):
    high = x.astype(bf16)
    return high, (x - high.astype(f32)).astype(bf16)


def tree_sum(values):
    values = list(values)
    while len(values) > 1:
        values = [a + b for a, b in zip(values[0::2], values[1::2])]
    return values[0]


def eye_mask(n):
    return lax.broadcasted_iota(jnp.int32, (n, n), 0) == lax.broadcasted_iota(jnp.int32, (n, n), 1)


def regularized(matrix):
    n = matrix.shape[0]
    eye = eye_mask(n)
    diagonal = jnp.where(eye, matrix, 0.0)
    ridge = ridge_share * jnp.sum(diagonal) / n
    return matrix + jnp.where(eye, ridge, 0.0)


def invert(matrix, x_ref, work_ref):
    n = matrix.shape[0]
    eye = eye_mask(n)
    diagonal = jnp.where(eye, matrix, 0.0)
    by_column = lax.rsqrt(jnp.sum(diagonal, axis=0, keepdims=True))
    by_row = lax.rsqrt(jnp.sum(diagonal, axis=1, keepdims=True))
    e1 = jnp.where(eye, 0.0, -(matrix * by_column) * by_row)
    e1_half = e1.astype(bf16)
    e2 = dot_fast(e1_half, e1_half)
    e2_half = e2.astype(bf16)
    e4 = dot_fast(e2_half, e2_half)
    e4_half = e4.astype(bf16)
    part = e1 + e2 + dot_fast(e1_half, e2_half)
    part = part + e4 + dot_fast(part.astype(bf16), e4_half)
    left = jnp.sum(e4 * e4)
    x_ref[...] = (part + jnp.where(eye, 1.0, 0.0)) * by_column * by_row

    @pl.when(jnp.logical_not(left < contraction_bound))
    def _():
        work_ref[...] = jnp.where(eye, 1.0, 0.0) - e1
        lane = lax.broadcasted_iota(jnp.int32, (n, n), 1)
        sublane = lax.broadcasted_iota(jnp.int32, (n, n), 0)
        lane_row = lax.broadcasted_iota(jnp.int32, (1, n), 1)

        def step(k, carry):
            work = work_ref[...]
            row = work_ref[pl.ds(k, 1), :]
            pivot = jnp.sum(jnp.where(lane_row == k, row, 0.0), axis=1, keepdims=True)
            column = jnp.sum(jnp.where(lane == k, work, 0.0), axis=1, keepdims=True)
            inverse = 1.0 / pivot
            new_row = jnp.where(lane_row == k, inverse, row * inverse)
            others = jnp.where(lane == k, 0.0, work) - column * new_row
            work_ref[...] = jnp.where(sublane == k, new_row, others)
            return carry

        lax.fori_loop(0, n, step, 0)
        x_ref[...] = work_ref[...] * by_column * by_row


def solve(right, matrix, inverse):
    first = dot(right, inverse)
    return first + dot(right - dot(first, matrix), inverse)


def place_of(axis):
    return lax.axis_index(axis)


def at_rows(block, rows):
    return pl.ds(pl.multiple_of(block * rows, rows), rows)


def space_kernel(tensor_ref, time_ref, species_ref, m_a_ref, side_ref):
    rows, species_count, steps = tensor_ref.shape
    time_high, time_low = split(time_ref[...])
    weights = jnp.concatenate([time_high, time_low, time_low, time_high], axis=0)
    species = species_ref[...]
    chunk = 8
    for start in range(0, rows, chunk):
        high, low = split(tensor_ref[start:start + chunk].reshape(chunk * species_count, steps))
        side = dot_fast(jnp.concatenate([high, low, high, low], axis=1), weights)
        side = side.reshape(chunk, species_count, side.shape[1])
        side_ref[start:start + chunk] = side
        m_a_ref[start:start + chunk, :] = jnp.sum(side * species[None], axis=1)


def transpose_kernel(after_ref, tensor_ref, high_ref, low_ref):
    rows, species_count, steps = tensor_ref.shape
    chunk = 8
    width = chunk * species_count
    for start in range(0, rows, chunk):
        turned = tensor_ref[start:start + chunk].reshape(width, steps).T
        high, low = split(turned)
        high_ref[:, start * species_count:start * species_count + width] = high
        low_ref[:, start * species_count:start * species_count + width] = low


def first_inverse_kernel(species_ref, own_ref, *refs):
    *halves, c_gram_ref, matrix_ref, inverse_ref, factor_ref, work_ref = refs
    block, core = place_of("tm"), place_of("space") % 2
    rows = own_ref.shape[0]
    half = rows // 2
    factor_ref[at_rows(block, rows), :] = own_ref[...]
    count = len(halves) // 2
    for j in range(1, count + 1):
        other = jnp.bitwise_xor(block, j) * 2
        factor_ref[at_rows(other + core, half), :] = halves[j - 1][...]
        factor_ref[at_rows(other + 1 - core, half), :] = halves[count + j - 1][...]
    c_gram = gram(factor_ref[...])
    c_gram_ref[...] = c_gram
    matrix = regularized(gram(species_ref[...]) * c_gram)
    matrix_ref[...] = matrix
    invert(matrix, inverse_ref, work_ref)


def space_solve_kernel(matrix_ref, inverse_ref, side_ref, *refs):
    *parts, packed_ref = refs
    m_a = tree_sum([part[...] for part in parts])
    raw = solve(m_a, matrix_ref[...], inverse_ref[...])
    rows, species_count, rank = side_ref.shape
    packed_ref[:rows, :] = raw
    total = jnp.zeros((species_count, rank), f32)
    for s in range(rows):
        total = total + side_ref[s] * packed_ref[pl.ds(s, 1), :]
    packed_ref[rows:, :] = total


def chip_sum_kernel(rows, *refs):
    *packed, raw_ref, m_b_ref = refs
    for j, block in enumerate(packed):
        raw_ref[j * rows:(j + 1) * rows, :] = block[:rows, :]
    m_b_ref[...] = tree_sum([block[rows:, :] for block in packed])


def space_gram_kernel(rows, c_gram_ref, mine_ref, partner_ref,
                      a_gram_ref, matrix_ref, scale_ref, raw_ref, out_ref, factor_ref):
    place = place_of("space")
    for j in range(mine_ref.shape[0] // rows):
        block = jnp.bitwise_xor(place, 2 * j)
        factor_ref[at_rows(block, rows), :] = mine_ref[j * rows:(j + 1) * rows, :]
        factor_ref[at_rows(jnp.bitwise_xor(block, 1), rows), :] = partner_ref[j * rows:(j + 1) * rows, :]
    raw_gram = gram(factor_ref[...])
    eye = eye_mask(raw_gram.shape[0])
    diagonal = jnp.where(eye, raw_gram, 0.0)
    total_rows = factor_ref.shape[0]
    by_column = lax.rsqrt(jnp.sum(diagonal, axis=0, keepdims=True) / total_rows + epsilon)
    by_row = lax.rsqrt(jnp.sum(diagonal, axis=1, keepdims=True) / total_rows + epsilon)
    scale_ref[...] = jnp.broadcast_to(by_column, scale_ref.shape)
    space = mine_ref[:rows, :] * by_column
    raw_ref[...] = space
    out_ref[...] = space
    a_gram = raw_gram * by_column * by_row
    a_gram_ref[...] = a_gram
    matrix_ref[...] = regularized(a_gram * c_gram_ref[...])


def inverse_kernel(matrix_ref, inverse_ref, work_ref):
    invert(matrix_ref[...], inverse_ref, work_ref)


def species_kernel(mine_ref, partner_ref, scale_ref, matrix_ref, inverse_ref, space_ref, high_ref, low_ref,
                   species_ref, out_ref, keep_ref, send_ref, product_ref):
    core = place_of("space") % 2
    m_b = (mine_ref[...] + partner_ref[...]) * scale_ref[0:1, :]
    raw = solve(m_b, matrix_ref[...], inverse_ref[...])
    species = raw * lax.rsqrt(jnp.mean(raw * raw, axis=0, keepdims=True) + epsilon)
    species_ref[...] = species
    out_ref[...] = species
    rows = space_ref.shape[0]
    species_count = species.shape[0]
    chunk = 8
    width = chunk * species_count
    total = jnp.zeros(product_ref.shape, f32)
    for start in range(0, rows, chunk):
        weights = species[None] * space_ref[start:start + chunk, :][:, None, :]
        weights_high, weights_low = split(weights.reshape(width, species.shape[1]))
        columns = slice(start * species_count, start * species_count + width)
        high, low = high_ref[:, columns], low_ref[:, columns]
        total = total + (dot_fast(high, weights_high) + (dot_fast(high, weights_low) + dot_fast(low, weights_high)))
    product_ref[...] = total
    half = keep_ref.shape[0]
    keep_ref[...] = product_ref[at_rows(core, half), :]
    send_ref[...] = product_ref[at_rows(1 - core, half), :]


def species_gram_kernel(a_gram_ref, species_ref, matrix_ref):
    matrix_ref[...] = regularized(a_gram_ref[...] * gram(species_ref[...]))


def time_solve_kernel(matrix_ref, inverse_ref, *refs):
    *parts, raw_ref, squares_ref = refs
    m_c = tree_sum([part[...] for part in parts])
    raw = solve(m_c, matrix_ref[...], inverse_ref[...])
    raw_ref[...] = raw
    squares_ref[...] = jnp.broadcast_to(jnp.sum(raw * raw, axis=0, keepdims=True), squares_ref.shape)


def time_scale_kernel(total_steps, mine_ref, partner_ref, my_squares_ref, partner_squares_ref, out_ref):
    core = place_of("space") % 2
    half = mine_ref.shape[0]
    squares = my_squares_ref[0:1, :] + partner_squares_ref[0:1, :]
    scale = lax.rsqrt(squares / total_steps + epsilon)
    out_ref[at_rows(core, half), :] = mine_ref[...] * scale
    out_ref[at_rows(1 - core, half), :] = partner_ref[...] * scale


def exchange(value, axis, step, count):
    return lax.ppermute(value, axis, [(i, i ^ step) for i in range(count)])


def run(kernel, name, outs, micros, scratch=()):
    call = pl.pallas_call(
        kernel,
        out_shape=outs,
        out_specs=[vmem] * len(outs),
        scratch_shapes=list(scratch),
        cost_estimate=pl.CostEstimate(flops=int(micros * flops_per_micro), bytes_accessed=0, transcendentals=0),
        compiler_params=pltpu.CompilerParams(vmem_limit_bytes=vmem_limit),
        name=name,
    )

    def placed(*operands):
        return call(*[pltpu.with_memory_space_constraint(x, pltpu.VMEM) for x in operands])

    return placed


def on_device(tensor, species_factor, time_factor):
    row_count, species_count, step_count = tensor.shape
    rank = species_factor.shape[1]
    devices = lax.axis_size("space")
    blocks = lax.axis_size("tm")
    chips = devices // 2
    total_rows = row_count * devices
    total_steps = step_count * blocks
    core = lax.axis_index("space") % 2

    def local(*dims):
        return pltpu.VMEM(dims, f32)

    def result(*dims):
        return jax.ShapeDtypeStruct(dims, f32)

    square = local(rank, rank)

    def over_time(value):
        return [value] + [exchange(value, "tm", j, blocks) for j in range(1, blocks)]

    def over_chips(value):
        return [value] + [exchange(value, "space", 2 * j, devices) for j in range(1, chips)]

    def to_partner(value):
        return exchange(value, "space", 1, devices)

    half_steps = step_count // 2
    own_half = lax.dynamic_slice_in_dim(time_factor, core * half_steps, half_steps)
    halves = over_time(own_half)[1:]
    m_a, side = run(
        space_kernel, "space_products", [local(row_count, rank), local(row_count, species_count, rank)], 4
    )(tensor, time_factor, species_factor)
    m_a_parts = over_time(m_a)
    partner_halves = [to_partner(half) for half in halves]
    c_gram, matrix, inverse = run(
        first_inverse_kernel, "first_inverse", [square] * 3, 4, [local(total_steps, rank), square]
    )(species_factor, time_factor, *halves, *partner_halves)

    (packed,) = run(space_solve_kernel, "space_solve", [local(row_count + species_count, rank)], 3)(
        matrix, inverse, side, *m_a_parts
    )
    packed_chips = over_chips(packed)
    turned = pltpu.VMEM((step_count, row_count * species_count), bf16)
    high, low = run(transpose_kernel, "turn_tensor", [turned] * 2, 3)(packed, tensor)
    raw_mine, m_b = run(
        lambda *refs: chip_sum_kernel(row_count, *refs),
        "chip_sum",
        [local(row_count * chips, rank), local(species_count, rank)],
        1,
    )(*packed_chips)
    raw_partner = to_partner(raw_mine)
    m_b_parts = over_time(m_b)
    a_gram, matrix, scale, space, space_out = run(
        lambda *refs: space_gram_kernel(row_count, *refs),
        "space_gram",
        [square, square, local(8, rank), local(row_count, rank), result(row_count, rank)],
        2,
        [local(total_rows, rank)],
    )(c_gram, raw_mine, raw_partner)
    m_b = tree_sum(m_b_parts)
    m_b_partner = to_partner(m_b)
    (inverse,) = run(inverse_kernel, "second_inverse", [square], 2, [square])(matrix)

    species, species_out, m_c_keep, m_c_send = run(
        species_kernel,
        "species_solve",
        [local(species_count, rank), result(species_count, rank), local(half_steps, rank), local(half_steps, rank)],
        4,
        [local(step_count, rank)],
    )(m_b, m_b_partner, scale, matrix, inverse, space, high, low)

    m_c_received = to_partner(m_c_send)
    (matrix,) = run(species_gram_kernel, "species_gram", [square], 1)(a_gram, species)
    m_c_parts = over_chips(m_c_keep + m_c_received)
    (inverse,) = run(inverse_kernel, "third_inverse", [square], 2, [square])(matrix)
    raw_time, squares = run(
        time_solve_kernel, "time_solve", [local(half_steps, rank), local(8, rank)], 2
    )(matrix, inverse, *m_c_parts)

    partner_time = to_partner(raw_time)
    squares = tree_sum(over_time(squares))
    partner_squares = to_partner(squares)
    (time_out,) = run(
        lambda *refs: time_scale_kernel(total_steps, *refs), "time_scale", [result(step_count, rank)], 1
    )(raw_time, partner_time, squares, partner_squares)
    return (space_out, species_out, time_out)


def solution(mesh):
    placed = (P("space", None, "tm"), P(), P("tm", None))
    return jax.shard_map(
        on_device,
        mesh=mesh,
        in_specs=placed,
        out_specs=(P("space", None), P(), P("tm", None)),
        check_vma=False,
    )
```

```python
import jax
import jax.numpy as jnp
from jax import lax
from jax.experimental import pallas as pl
from jax.experimental.pallas import tpu as pltpu
from jax.sharding import PartitionSpec as P


ridge_share = 0.1
epsilon = 1e-06
contraction_bound = 1e-3
highest = lax.Precision.HIGHEST
f32 = jnp.float32
bf16 = jnp.bfloat16

vmem = pl.BlockSpec(memory_space=pltpu.VMEM)
flops_per_micro = 1e9
vmem_limit = 24 * 1024 * 1024


def dot(a, b, dims=((1,), (0,))):
    return lax.dot_general(a, b, (dims, ((), ())), precision=highest, preferred_element_type=f32)


def dot_fast(a, b, dims=((1,), (0,))):
    return lax.dot_general(a, b, (dims, ((), ())), preferred_element_type=f32)


def gram(factor):
    return dot(factor, factor, ((0,), (0,)))


def split(x):
    high = x.astype(bf16)
    return high, (x - high.astype(f32)).astype(bf16)


def tree_sum(values):
    values = list(values)
    while len(values) > 1:
        values = [a + b for a, b in zip(values[0::2], values[1::2])]
    return values[0]


def eye_mask(n):
    return lax.broadcasted_iota(jnp.int32, (n, n), 0) == lax.broadcasted_iota(jnp.int32, (n, n), 1)


def regularized(matrix):
    n = matrix.shape[0]
    eye = eye_mask(n)
    diagonal = jnp.where(eye, matrix, 0.0)
    ridge = ridge_share * jnp.sum(diagonal) / n
    return matrix + jnp.where(eye, ridge, 0.0)


def invert(matrix, x_ref, work_ref):
    n = matrix.shape[0]
    eye = eye_mask(n)
    diagonal = jnp.where(eye, matrix, 0.0)
    by_column = lax.rsqrt(jnp.sum(diagonal, axis=0, keepdims=True))
    by_row = lax.rsqrt(jnp.sum(diagonal, axis=1, keepdims=True))
    e1 = jnp.where(eye, 0.0, -(matrix * by_column) * by_row)
    e1_half = e1.astype(bf16)
    e2 = dot_fast(e1_half, e1_half)
    e2_half = e2.astype(bf16)
    e4 = dot_fast(e2_half, e2_half)
    e4_half = e4.astype(bf16)
    part = e1 + e2 + dot_fast(e1_half, e2_half)
    part = part + e4 + dot_fast(part.astype(bf16), e4_half)
    left = jnp.sum(e4 * e4)
    x_ref[...] = (part + jnp.where(eye, 1.0, 0.0)) * by_column * by_row

    @pl.when(jnp.logical_not(left < contraction_bound))
    def _():
        work_ref[...] = jnp.where(eye, 1.0, 0.0) - e1
        lane = lax.broadcasted_iota(jnp.int32, (n, n), 1)
        sublane = lax.broadcasted_iota(jnp.int32, (n, n), 0)
        lane_row = lax.broadcasted_iota(jnp.int32, (1, n), 1)

        def step(k, carry):
            work = work_ref[...]
            row = work_ref[pl.ds(k, 1), :]
            pivot = jnp.sum(jnp.where(lane_row == k, row, 0.0), axis=1, keepdims=True)
            column = jnp.sum(jnp.where(lane == k, work, 0.0), axis=1, keepdims=True)
            inverse = 1.0 / pivot
            new_row = jnp.where(lane_row == k, inverse, row * inverse)
            others = jnp.where(lane == k, 0.0, work) - column * new_row
            work_ref[...] = jnp.where(sublane == k, new_row, others)
            return carry

        lax.fori_loop(0, n, step, 0)
        x_ref[...] = work_ref[...] * by_column * by_row


def solve(right, matrix, inverse):
    first = dot(right, inverse)
    return first + dot(right - dot(first, matrix), inverse)


def place_of(axis):
    return lax.axis_index(axis)


def at_rows(block, rows):
    return pl.ds(pl.multiple_of(block * rows, rows), rows)


def space_kernel(chunk, tensor_hbm, time_hbm, species_hbm,
                 m_a_ref, side_ref, tensor_ref, time_ref, species_ref, arrived):
    rows, species_count, steps = tensor_ref.shape
    copies = [
        pltpu.make_async_copy(time_hbm, time_ref, arrived.at[0]),
        pltpu.make_async_copy(species_hbm, species_ref, arrived.at[1]),
    ]
    for i in range(rows // chunk):
        block = pl.ds(i * chunk, chunk)
        copies.append(pltpu.make_async_copy(tensor_hbm.at[block], tensor_ref.at[block], arrived.at[2 + i]))
    for copy in copies:
        copy.start()
    copies[0].wait()
    copies[1].wait()
    time_high, time_low = split(time_ref[...])
    weights = jnp.concatenate([time_high, time_low, time_low, time_high], axis=0)
    species = species_ref[...]
    for i in range(rows // chunk):
        copies[2 + i].wait()
        start = i * chunk
        high, low = split(tensor_ref[start:start + chunk].reshape(chunk * species_count, steps))
        side = dot_fast(jnp.concatenate([high, low, high, low], axis=1), weights)
        side = side.reshape(chunk, species_count, side.shape[1])
        side_ref[start:start + chunk] = side
        m_a_ref[start:start + chunk, :] = jnp.sum(side * species[None], axis=1)


def pack_kernel(after_ref, *refs):
    *parts, out_ref = refs
    rows = parts[0].shape[0]
    for j, part in enumerate(parts):
        out_ref[j * rows:(j + 1) * rows, :] = part[...]


def sum_kernel(*refs):
    *parts, out_ref = refs
    out_ref[...] = tree_sum([part[...] for part in parts])


def transpose_kernel(after_ref, tensor_ref, high_ref, low_ref):
    rows, species_count, steps = tensor_ref.shape
    chunk = 8
    width = chunk * species_count
    for start in range(0, rows, chunk):
        turned = tensor_ref[start:start + chunk].reshape(width, steps).T
        high, low = split(turned)
        high_ref[:, start * species_count:start * species_count + width] = high
        low_ref[:, start * species_count:start * species_count + width] = low


def first_inverse_kernel(species_ref, own_ref, mine_ref, partner_ref,
                         c_gram_ref, matrix_ref, inverse_ref, factor_ref, work_ref):
    block, core = place_of("tm"), place_of("space") % 2
    rows = own_ref.shape[0]
    half = rows // 2
    factor_ref[at_rows(block, rows), :] = own_ref[...]
    for j in range(mine_ref.shape[0] // half):
        other = jnp.bitwise_xor(block, j + 1) * 2
        factor_ref[at_rows(other + core, half), :] = mine_ref[j * half:(j + 1) * half, :]
        factor_ref[at_rows(other + 1 - core, half), :] = partner_ref[j * half:(j + 1) * half, :]
    c_gram = gram(factor_ref[...])
    c_gram_ref[...] = c_gram
    matrix = regularized(gram(species_ref[...]) * c_gram)
    matrix_ref[...] = matrix
    invert(matrix, inverse_ref, work_ref)


def space_solve_kernel(matrix_ref, inverse_ref, side_ref, *refs):
    *parts, raw_ref, m_b_ref = refs
    m_a = tree_sum([part[...] for part in parts])
    raw_ref[...] = solve(m_a, matrix_ref[...], inverse_ref[...])
    total = jnp.zeros(m_b_ref.shape, f32)
    for s in range(side_ref.shape[0]):
        total = total + side_ref[s] * raw_ref[pl.ds(s, 1), :]
    m_b_ref[...] = total


def space_gram_kernel(rows, c_gram_ref, mine_ref, partner_ref,
                      a_gram_ref, matrix_ref, scale_ref, raw_ref, out_ref, factor_ref):
    place = place_of("space")
    for j in range(mine_ref.shape[0] // rows):
        block = jnp.bitwise_xor(place, 2 * j)
        factor_ref[at_rows(block, rows), :] = mine_ref[j * rows:(j + 1) * rows, :]
        factor_ref[at_rows(jnp.bitwise_xor(block, 1), rows), :] = partner_ref[j * rows:(j + 1) * rows, :]
    raw_gram = gram(factor_ref[...])
    eye = eye_mask(raw_gram.shape[0])
    diagonal = jnp.where(eye, raw_gram, 0.0)
    total_rows = factor_ref.shape[0]
    by_column = lax.rsqrt(jnp.sum(diagonal, axis=0, keepdims=True) / total_rows + epsilon)
    by_row = lax.rsqrt(jnp.sum(diagonal, axis=1, keepdims=True) / total_rows + epsilon)
    scale_ref[...] = jnp.broadcast_to(by_column, scale_ref.shape)
    space = mine_ref[:rows, :] * by_column
    raw_ref[...] = space
    out_ref[...] = space
    a_gram = raw_gram * by_column * by_row
    a_gram_ref[...] = a_gram
    matrix_ref[...] = regularized(a_gram * c_gram_ref[...])


def inverse_kernel(matrix_ref, inverse_ref, work_ref):
    invert(matrix_ref[...], inverse_ref, work_ref)


def species_kernel(mine_ref, partner_ref, scale_ref, matrix_ref, inverse_ref, space_ref, high_ref, low_ref,
                   species_ref, out_ref, keep_ref, send_ref, product_ref):
    core = place_of("space") % 2
    m_b = (mine_ref[...] + partner_ref[...]) * scale_ref[0:1, :]
    raw = solve(m_b, matrix_ref[...], inverse_ref[...])
    species = raw * lax.rsqrt(jnp.mean(raw * raw, axis=0, keepdims=True) + epsilon)
    species_ref[...] = species
    out_ref[...] = species
    rows = space_ref.shape[0]
    species_count = species.shape[0]
    chunk = 8
    width = chunk * species_count
    total = jnp.zeros(product_ref.shape, f32)
    for start in range(0, rows, chunk):
        weights = species[None] * space_ref[start:start + chunk, :][:, None, :]
        weights_high, weights_low = split(weights.reshape(width, species.shape[1]))
        columns = slice(start * species_count, start * species_count + width)
        high, low = high_ref[:, columns], low_ref[:, columns]
        total = total + (dot_fast(high, weights_high) + (dot_fast(high, weights_low) + dot_fast(low, weights_high)))
    product_ref[...] = total
    half = keep_ref.shape[0]
    keep_ref[...] = product_ref[at_rows(core, half), :]
    send_ref[...] = product_ref[at_rows(1 - core, half), :]


def species_gram_kernel(a_gram_ref, species_ref, matrix_ref):
    matrix_ref[...] = regularized(a_gram_ref[...] * gram(species_ref[...]))


def time_solve_kernel(matrix_ref, inverse_ref, mine_ref, partner_ref, raw_ref, squares_ref, m_c_ref):
    core = place_of("space") % 2
    half = mine_ref.shape[0]
    m_c_ref[at_rows(core, half), :] = mine_ref[...]
    m_c_ref[at_rows(1 - core, half), :] = partner_ref[...]
    raw = solve(m_c_ref[...], matrix_ref[...], inverse_ref[...])
    raw_ref[...] = raw
    squares_ref[...] = jnp.broadcast_to(jnp.sum(raw * raw, axis=0, keepdims=True), squares_ref.shape)


def time_scale_kernel(total_steps, raw_ref, *refs):
    *parts, out_ref = refs
    squares = tree_sum([part[0:1, :] for part in parts])
    out_ref[...] = raw_ref[...] * lax.rsqrt(squares / total_steps + epsilon)


def exchange(value, axis, step, count):
    return lax.ppermute(value, axis, [(i, i ^ step) for i in range(count)])


def run(kernel, outs, micros, scratch=()):
    call = pl.pallas_call(
        kernel,
        out_shape=outs,
        out_specs=[vmem] * len(outs),
        scratch_shapes=list(scratch),
        cost_estimate=pl.CostEstimate(flops=int(micros * flops_per_micro), bytes_accessed=0, transcendentals=0),
        compiler_params=pltpu.CompilerParams(vmem_limit_bytes=vmem_limit),
    )

    def placed(*operands):
        return call(*[pltpu.with_memory_space_constraint(x, pltpu.VMEM) for x in operands])

    return placed


def on_device(tensor, species_factor, time_factor):
    row_count, species_count, step_count = tensor.shape
    rank = species_factor.shape[1]
    devices = lax.axis_size("space")
    blocks = lax.axis_size("tm")
    chips = devices // 2
    total_rows = row_count * devices
    total_steps = step_count * blocks
    core = lax.axis_index("space") % 2

    def local(*dims):
        return pltpu.VMEM(dims, f32)

    def result(*dims):
        return jax.ShapeDtypeStruct(dims, f32)

    square = local(rank, rank)

    def over_time(value):
        return [value] + [exchange(value, "tm", j, blocks) for j in range(1, blocks)]

    def over_chips(value):
        return [value] + [exchange(value, "space", 2 * j, devices) for j in range(1, chips)]

    def to_partner(value):
        return exchange(value, "space", 1, devices)

    def pack(after, parts):
        return run(pack_kernel, [local(len(parts) * parts[0].shape[0], rank)], 0.3)(after, *parts)[0]

    def add(parts):
        return run(sum_kernel, [local(*parts[0].shape)], 0.3)(*parts)[0]

    half_steps = step_count // 2
    own_half = lax.dynamic_slice_in_dim(time_factor, core * half_steps, half_steps)
    halves = over_time(own_half)[1:]

    chunk = 8
    outside = pl.BlockSpec(memory_space=pltpu.HBM)
    m_a, side, tensor_here, time_here, species_here = pl.pallas_call(
        lambda *refs: space_kernel(chunk, *refs),
        in_specs=[outside] * 3,
        out_specs=[vmem] * 5,
        out_shape=[
            local(row_count, rank),
            local(row_count, species_count, rank),
            local(row_count, species_count, step_count),
            local(step_count, rank),
            local(species_count, rank),
        ],
        scratch_shapes=[pltpu.SemaphoreType.DMA((2 + row_count // chunk,))],
        cost_estimate=pl.CostEstimate(flops=int(3 * flops_per_micro), bytes_accessed=0, transcendentals=0),
        compiler_params=pltpu.CompilerParams(vmem_limit_bytes=vmem_limit),
        name="space_products",
    )(*[pltpu.with_memory_space_constraint(x, pltpu.HBM) for x in (tensor, time_factor, species_factor)])
    m_a_parts = over_time(m_a)

    halves = pack(m_a, halves)
    partner_halves = to_partner(halves)
    c_gram, matrix, inverse = run(
        first_inverse_kernel, [square] * 3, 2, [local(total_steps, rank), square]
    )(species_here, time_here, halves, partner_halves)

    raw, m_b = run(
        space_solve_kernel, [local(row_count, rank), local(species_count, rank)], 1
    )(matrix, inverse, side, *m_a_parts)
    m_b_parts = over_time(m_b)
    raw_chips = over_chips(raw)
    turned = pltpu.VMEM((step_count, row_count * species_count), bf16)
    high, low = run(transpose_kernel, [turned] * 2, 1)(m_b, tensor_here)
    m_b_parts = over_chips(add(m_b_parts))
    raw_mine = pack(m_b, raw_chips)
    raw_partner = to_partner(raw_mine)
    a_gram, matrix, scale, space, space_out = run(
        lambda *refs: space_gram_kernel(row_count, *refs),
        [square, square, local(8, rank), local(row_count, rank), result(row_count, rank)],
        1.5,
        [local(total_rows, rank)],
    )(c_gram, raw_mine, raw_partner)
    (inverse,) = run(inverse_kernel, [square], 1, [square])(matrix)
    m_b = add(m_b_parts)
    m_b_partner = to_partner(m_b)

    species, species_out, m_c_keep, m_c_send = run(
        species_kernel,
        [local(species_count, rank), result(species_count, rank), local(half_steps, rank), local(half_steps, rank)],
        3,
        [local(step_count, rank)],
    )(m_b, m_b_partner, scale, matrix, inverse, space, high, low)

    m_c_received = to_partner(m_c_send)
    (matrix,) = run(species_gram_kernel, [square], 0.5)(a_gram, species)
    m_c_parts = over_chips(add([m_c_keep, m_c_received]))
    (inverse,) = run(inverse_kernel, [square], 1, [square])(matrix)
    m_c = add(m_c_parts)
    m_c_partner = to_partner(m_c)
    raw_time, squares = run(
        time_solve_kernel, [local(step_count, rank), local(8, rank)], 1, [local(step_count, rank)]
    )(matrix, inverse, m_c, m_c_partner)

    squares = over_time(squares)
    (time_out,) = run(
        lambda *refs: time_scale_kernel(total_steps, *refs), [result(step_count, rank)], 0.5
    )(raw_time, *squares)
    return (space_out, species_out, time_out)


def solution(mesh):
    placed = (P("space", None, "tm"), P(), P("tm", None))
    return jax.shard_map(
        on_device,
        mesh=mesh,
        in_specs=placed,
        out_specs=(P("space", None), P(), P("tm", None)),
        check_vma=False,
    )
```

```python
import jax
import jax.numpy as jnp
from jax import lax
from jax.experimental import pallas as pl
from jax.experimental.pallas import tpu as pltpu
from jax.sharding import PartitionSpec as P


TIME_PAIR = True
RAW_PAIR = True
MB_HALF = True
ridge_share = 0.1
epsilon = 1e-06
contraction_bound = 1e-3
highest = lax.Precision.HIGHEST
f32 = jnp.float32
bf16 = jnp.bfloat16

vmem = pl.BlockSpec(memory_space=pltpu.VMEM)
flops_per_micro = 1e9
vmem_limit = 24 * 1024 * 1024


def dot(a, b, dims=((1,), (0,))):
    return lax.dot_general(a, b, (dims, ((), ())), precision=highest, preferred_element_type=f32)


def dot_fast(a, b, dims=((1,), (0,))):
    return lax.dot_general(a, b, (dims, ((), ())), preferred_element_type=f32)


def gram(factor):
    return dot(factor, factor, ((0,), (0,)))


def split(x):
    high = x.astype(bf16)
    return high, (x - high.astype(f32)).astype(bf16)


def tree_sum(values):
    values = list(values)
    while len(values) > 1:
        values = [a + b for a, b in zip(values[0::2], values[1::2])]
    return values[0]


def eye_mask(n):
    return lax.broadcasted_iota(jnp.int32, (n, n), 0) == lax.broadcasted_iota(jnp.int32, (n, n), 1)


def regularized(matrix):
    n = matrix.shape[0]
    eye = eye_mask(n)
    diagonal = jnp.where(eye, matrix, 0.0)
    ridge = ridge_share * jnp.sum(diagonal) / n
    return matrix + jnp.where(eye, ridge, 0.0)


def invert(matrix, x_ref, work_ref):
    n = matrix.shape[0]
    eye = eye_mask(n)
    diagonal = jnp.where(eye, matrix, 0.0)
    by_column = lax.rsqrt(jnp.sum(diagonal, axis=0, keepdims=True))
    by_row = lax.rsqrt(jnp.sum(diagonal, axis=1, keepdims=True))
    e1 = jnp.where(eye, 0.0, -(matrix * by_column) * by_row)
    e1_half = e1.astype(bf16)
    e2 = dot_fast(e1_half, e1_half)
    e2_half = e2.astype(bf16)
    e4 = dot_fast(e2_half, e2_half)
    e4_half = e4.astype(bf16)
    part = e1 + e2 + dot_fast(e1_half, e2_half)
    part = part + e4 + dot_fast(part.astype(bf16), e4_half)
    left = jnp.sum(e4 * e4)
    x_ref[...] = (part + jnp.where(eye, 1.0, 0.0)) * by_column * by_row

    @pl.when(jnp.logical_not(left < contraction_bound))
    def _():
        work_ref[...] = jnp.where(eye, 1.0, 0.0) - e1
        lane = lax.broadcasted_iota(jnp.int32, (n, n), 1)
        sublane = lax.broadcasted_iota(jnp.int32, (n, n), 0)
        lane_row = lax.broadcasted_iota(jnp.int32, (1, n), 1)

        def step(k, carry):
            work = work_ref[...]
            row = work_ref[pl.ds(k, 1), :]
            pivot = jnp.sum(jnp.where(lane_row == k, row, 0.0), axis=1, keepdims=True)
            column = jnp.sum(jnp.where(lane == k, work, 0.0), axis=1, keepdims=True)
            inverse = 1.0 / pivot
            new_row = jnp.where(lane_row == k, inverse, row * inverse)
            others = jnp.where(lane == k, 0.0, work) - column * new_row
            work_ref[...] = jnp.where(sublane == k, new_row, others)
            return carry

        lax.fori_loop(0, n, step, 0)
        x_ref[...] = work_ref[...] * by_column * by_row


def solve(right, matrix, inverse):
    first = dot(right, inverse)
    return first + dot(right - dot(first, matrix), inverse)


def place_of(axis):
    return lax.axis_index(axis)


def at_rows(block, rows):
    return pl.ds(pl.multiple_of(block * rows, rows), rows)


def load_kernel(time_hbm, species_hbm, half_ref, time_ref, species_ref, arrived):
    half = half_ref.shape[0]
    copies = [
        pltpu.make_async_copy(time_hbm.at[at_rows(place_of("space") % 2, half)], half_ref, arrived.at[0]),
        pltpu.make_async_copy(time_hbm, time_ref, arrived.at[1]),
        pltpu.make_async_copy(species_hbm, species_ref, arrived.at[2]),
    ]
    for copy in copies:
        copy.start()
    for copy in copies:
        copy.wait()


def space_kernel(tensor_ref, time_ref, species_ref, m_a_ref, side_ref):
    species = species_ref[...]
    species_count = species.shape[0]
    time_high, time_low = split(time_ref[...])
    weights = jnp.concatenate([time_high, time_low, time_low, time_high], axis=0)
    chunk = 8
    height = chunk * species_count
    for start in range(0, tensor_ref.shape[0], height):
        high, low = split(tensor_ref[start:start + height, :])
        side = dot_fast(jnp.concatenate([high, low, high, low], axis=1), weights)
        side = side.reshape(chunk, species_count, side.shape[1])
        at = start // species_count
        side_ref[at:at + chunk] = side
        m_a_ref[at:at + chunk, :] = jnp.sum(side * species[None], axis=1)


def pack_kernel(after_ref, *refs):
    *parts, out_ref = refs
    at = 0
    for part in parts:
        out_ref[at:at + part.shape[0], :] = part[...]
        at += part.shape[0]


def peers(count, paired):
    if not paired:
        return [], list(range(1, count))
    return [(j, j + 1) for j in range(1, count - 1, 2)], [count - 1]


def place_blocks(factor_ref, place, core, own_ref, mine_ref, partner_ref, paired):
    rows = own_ref.shape[0]
    half = rows // 2
    factor_ref[at_rows(place, rows), :] = own_ref[...]
    pairs, shared = peers(factor_ref.shape[0] // rows, paired)
    for i, (first, second) in enumerate(pairs):
        step = second - first
        taken = slice(i * rows, (i + 1) * rows)
        factor_ref[at_rows(jnp.bitwise_xor(place, first + core * step), rows), :] = mine_ref[taken, :]
        factor_ref[at_rows(jnp.bitwise_xor(place, second - core * step), rows), :] = partner_ref[taken, :]
    for i, step in enumerate(shared):
        start = len(pairs) * rows + i * half
        taken = slice(start, start + half)
        at = jnp.bitwise_xor(place, step) * 2
        factor_ref[at_rows(at + core, half), :] = mine_ref[taken, :]
        factor_ref[at_rows(at + 1 - core, half), :] = partner_ref[taken, :]


def sum_kernel(*refs):
    *parts, out_ref = refs
    out_ref[...] = tree_sum([part[...] for part in parts])


def time_side_kernel(species_count, raw_ref, tensor_ref, side_ref):
    rows = raw_ref.shape[0]
    raw_high, raw_low = split(raw_ref[...])
    weights = jnp.concatenate([raw_high, raw_high, raw_low, raw_low], axis=0)
    for p in range(species_count):
        high, low = split(tensor_ref[pl.ds(p, rows, stride=species_count), :])
        side_ref[p] = dot_fast(jnp.concatenate([high, low, high, low], axis=0), weights, ((0,), (0,)))


def first_inverse_kernel(species_ref, own_ref, mine_ref, partner_ref,
                         c_gram_ref, matrix_ref, inverse_ref, factor_ref, work_ref):
    place_blocks(factor_ref, place_of("tm"), place_of("space") % 2, own_ref, mine_ref, partner_ref, TIME_PAIR)
    c_gram = gram(factor_ref[...])
    c_gram_ref[...] = c_gram
    matrix = regularized(gram(species_ref[...]) * c_gram)
    matrix_ref[...] = matrix
    invert(matrix, inverse_ref, work_ref)


def space_solve_kernel(matrix_ref, inverse_ref, side_ref, *refs):
    *parts, raw_ref, keep_ref, send_ref, m_b_ref = refs
    core = place_of("space") % 2
    m_a = tree_sum([part[...] for part in parts])
    raw = solve(m_a, matrix_ref[...], inverse_ref[...])
    raw_ref[...] = raw
    rows = raw.shape[0]
    send_ref[:rows, :] = raw
    total = jnp.zeros(m_b_ref.shape, f32)
    for s in range(rows):
        total = total + side_ref[s] * raw_ref[pl.ds(s, 1), :]
    m_b_ref[...] = total
    half = keep_ref.shape[0]
    if MB_HALF:
        keep_ref[...] = m_b_ref[at_rows(core, half), :]
        send_ref[rows:, :] = m_b_ref[at_rows(1 - core, half), :]
    else:
        keep_ref[...] = total
        send_ref[rows:, :] = total


def chip_kernel(raw_ref, keep_ref, received_ref, block_ref, m_b_ref):
    core = place_of("space") % 2
    rows = raw_ref.shape[0]
    block_ref[at_rows(core, rows), :] = raw_ref[...]
    block_ref[at_rows(1 - core, rows), :] = received_ref[:rows, :]
    m_b_ref[...] = keep_ref[...] + received_ref[rows:, :]


def space_gram_kernel(c_gram_ref, own_ref, mine_ref, partner_ref,
                      a_gram_ref, matrix_ref, scale_ref, out_ref, factor_ref):
    place = place_of("space")
    place_blocks(factor_ref, place // 2, place % 2, own_ref, mine_ref, partner_ref, RAW_PAIR)
    raw_gram = gram(factor_ref[...])
    eye = eye_mask(raw_gram.shape[0])
    diagonal = jnp.where(eye, raw_gram, 0.0)
    total_rows = factor_ref.shape[0]
    by_column = lax.rsqrt(jnp.sum(diagonal, axis=0, keepdims=True) / total_rows + epsilon)
    by_row = lax.rsqrt(jnp.sum(diagonal, axis=1, keepdims=True) / total_rows + epsilon)
    scale_ref[...] = jnp.broadcast_to(by_column, scale_ref.shape)
    out_ref[...] = own_ref[at_rows(place % 2, out_ref.shape[0]), :] * by_column
    a_gram = raw_gram * by_column * by_row
    a_gram_ref[...] = a_gram
    matrix_ref[...] = regularized(a_gram * c_gram_ref[...])


def inverse_kernel(matrix_ref, inverse_ref, work_ref):
    invert(matrix_ref[...], inverse_ref, work_ref)


def species_kernel(scale_ref, matrix_ref, inverse_ref, side_ref, *refs):
    *parts, species_ref, out_ref, keep_ref, send_ref, scaled_ref = refs
    core = place_of("space") % 2
    scale = scale_ref[0:1, :]
    if MB_HALF:
        mine_ref, partner_ref = parts
        half = mine_ref.shape[0]
        scaled_ref[at_rows(core, half), :] = mine_ref[...]
        scaled_ref[at_rows(1 - core, half), :] = partner_ref[...]
        m_b = scaled_ref[...] * scale
    else:
        m_b = tree_sum([part[...] for part in parts]) * scale
    raw = solve(m_b, matrix_ref[...], inverse_ref[...])
    species = raw * lax.rsqrt(jnp.mean(raw * raw, axis=0, keepdims=True) + epsilon)
    species_ref[...] = species
    out_ref[...] = species
    scaled_ref[...] = species * scale
    half = keep_ref.shape[0]
    for ref, block in ((send_ref, 1 - core), (keep_ref, core)):
        total = jnp.zeros(ref.shape, f32)
        for p in range(side_ref.shape[0]):
            total = total + side_ref[p, at_rows(block, half), :] * scaled_ref[p:p + 1, :]
        ref[...] = total


def species_gram_kernel(a_gram_ref, species_ref, matrix_ref):
    matrix_ref[...] = regularized(a_gram_ref[...] * gram(species_ref[...]))


def time_solve_kernel(matrix_ref, inverse_ref, mine_ref, partner_ref, raw_ref, squares_ref, m_c_ref):
    core = place_of("space") % 2
    half = mine_ref.shape[0]
    m_c_ref[at_rows(core, half), :] = mine_ref[...]
    m_c_ref[at_rows(1 - core, half), :] = partner_ref[...]
    raw = solve(m_c_ref[...], matrix_ref[...], inverse_ref[...])
    raw_ref[...] = raw
    squares_ref[...] = jnp.broadcast_to(jnp.sum(raw * raw, axis=0, keepdims=True), squares_ref.shape)


def time_scale_kernel(total_steps, raw_ref, *refs):
    *parts, out_ref = refs
    squares = tree_sum([part[0:1, :] for part in parts])
    out_ref[...] = raw_ref[...] * lax.rsqrt(squares / total_steps + epsilon)


def exchange(value, axis, step, count):
    return lax.ppermute(value, axis, [(i, i ^ step) for i in range(count)])


def run(kernel, outs, micros, scratch=()):
    call = pl.pallas_call(
        kernel,
        out_shape=outs,
        out_specs=[vmem] * len(outs),
        scratch_shapes=list(scratch),
        cost_estimate=pl.CostEstimate(flops=int(micros * flops_per_micro), bytes_accessed=0, transcendentals=0),
        compiler_params=pltpu.CompilerParams(vmem_limit_bytes=vmem_limit),
    )

    def placed(*operands):
        return call(*[pltpu.with_memory_space_constraint(x, pltpu.VMEM) for x in operands])

    return placed


def on_device(tensor, species_factor, time_factor):
    row_count, species_count, step_count = tensor.shape
    rank = species_factor.shape[1]
    devices = lax.axis_size("space")
    blocks = lax.axis_size("tm")
    chips = devices // 2
    total_rows = row_count * devices
    total_steps = step_count * blocks

    def local(*dims):
        return pltpu.VMEM(dims, f32)

    def result(*dims):
        return jax.ShapeDtypeStruct(dims, f32)

    square = local(rank, rank)

    def over_time(value):
        return [value] + [exchange(value, "tm", j, blocks) for j in range(1, blocks)]

    def over_chips(value):
        return [value] + [exchange(value, "space", 2 * j, devices) for j in range(1, chips)]

    def to_partner(value):
        return exchange(value, "space", 1, devices)

    def block_from(block, half, axis):
        pairs, shared = peers(blocks, TIME_PAIR) if axis == "tm" else peers(chips, RAW_PAIR)
        received = []
        for steps in pairs:
            if axis == "tm":
                turns = [
                    (s * blocks + t, s * blocks + (t ^ steps[s % 2])) for s in range(devices) for t in range(blocks)
                ]
                received.append(lax.ppermute(block, ("space", "tm"), turns))
            else:
                turns = [(s, s ^ (2 * steps[s % 2])) for s in range(devices)]
                received.append(lax.ppermute(block, "space", turns))
        for j in shared:
            step, count = (j, blocks) if axis == "tm" else (2 * j, devices)
            received.append(exchange(half, axis, step, count))
        return received

    def pack(after, parts):
        return run(pack_kernel, [local(sum(part.shape[0] for part in parts), rank)], 0.3)(after, *parts)[0]

    def add(parts):
        return run(sum_kernel, [local(*parts[0].shape)], 0.3)(*parts)[0]

    half_steps = step_count // 2
    half_species = species_count // 2 if MB_HALF else species_count

    outside = pl.BlockSpec(memory_space=pltpu.HBM)
    time_half, time_here, species_here = pl.pallas_call(
        load_kernel,
        in_specs=[outside] * 2,
        out_specs=[vmem] * 3,
        out_shape=[local(half_steps, rank), local(step_count, rank), local(species_count, rank)],
        scratch_shapes=[pltpu.SemaphoreType.DMA((3,))],
        cost_estimate=pl.CostEstimate(flops=int(10 * flops_per_micro), bytes_accessed=10**8, transcendentals=0),
        compiler_params=pltpu.CompilerParams(vmem_limit_bytes=vmem_limit),
        name="load_factors",
    )(*[pltpu.with_memory_space_constraint(x, pltpu.HBM) for x in (time_factor, species_factor)])
    received = block_from(time_here, time_half, "tm")
    m_a, side = run(
        space_kernel, [local(row_count, rank), local(row_count, species_count, rank)], 2
    )(tensor.reshape(row_count * species_count, step_count), time_here, species_here)
    m_a_parts = over_time(m_a)

    mine = pack(m_a, received)
    partner = to_partner(mine)
    c_gram, matrix, inverse = run(
        first_inverse_kernel, [square] * 3, 2, [local(total_steps, rank), square]
    )(species_here, time_here, mine, partner)

    raw, keep, send = run(
        space_solve_kernel,
        [local(row_count, rank), local(half_species, rank), local(row_count + half_species, rank)],
        1,
        [local(species_count, rank)],
    )(matrix, inverse, side, *m_a_parts)
    received = to_partner(send)
    (time_side,) = run(
        lambda *refs: time_side_kernel(species_count, *refs), [local(species_count, step_count, rank)], 2
    )(raw, tensor.reshape(row_count * species_count, step_count))
    chip_block, m_b = run(chip_kernel, [local(2 * row_count, rank), local(half_species, rank)], 0.3)(
        raw, keep, received
    )
    m_b_parts = over_time(m_b)
    raw_blocks = block_from(chip_block, raw, "space")
    m_b_parts = over_chips(add(m_b_parts))
    mine = pack(m_b, raw_blocks)
    partner = to_partner(mine)
    if MB_HALF:
        m_b = add(m_b_parts)
        m_b_parts = [m_b, to_partner(m_b)]
    a_gram, matrix, scale, space_out = run(
        space_gram_kernel, [square, square, local(8, rank), result(row_count, rank)], 1.5, [local(total_rows, rank)]
    )(c_gram, chip_block, mine, partner)
    (inverse,) = run(inverse_kernel, [square], 1, [square])(matrix)

    species, species_out, m_c_keep, m_c_send = run(
        species_kernel,
        [local(species_count, rank), result(species_count, rank), local(half_steps, rank), local(half_steps, rank)],
        1.5,
        [local(species_count, rank)],
    )(scale, matrix, inverse, time_side, *m_b_parts)

    m_c_received = to_partner(m_c_send)
    (matrix,) = run(species_gram_kernel, [square], 0.5)(a_gram, species)
    m_c_parts = over_chips(add([m_c_keep, m_c_received]))
    (inverse,) = run(inverse_kernel, [square], 1, [square])(matrix)
    m_c = add(m_c_parts)
    m_c_partner = to_partner(m_c)
    raw_time, squares = run(
        time_solve_kernel, [local(step_count, rank), local(8, rank)], 1, [local(step_count, rank)]
    )(matrix, inverse, m_c, m_c_partner)

    squares = over_time(squares)
    (time_out,) = run(
        lambda *refs: time_scale_kernel(total_steps, *refs), [result(step_count, rank)], 0.5
    )(raw_time, *squares)
    return (space_out, species_out, time_out)


def solution(mesh):
    placed = (P("space", None, "tm"), P(), P("tm", None))
    return jax.shard_map(
        on_device,
        mesh=mesh,
        in_specs=placed,
        out_specs=(P("space", None), P(), P("tm", None)),
        check_vma=False,
    )
```

```python
import jax
import jax.numpy as jnp
from jax import lax
from jax.experimental import pallas as pl
from jax.experimental.pallas import tpu as pltpu
from jax.sharding import PartitionSpec as P


TIME_PAIR = True
RAW_PAIR = True
MB_HALF = True
MB_TREE = False
EARLY = 5
ridge_share = 0.1
epsilon = 1e-06
contraction_bound = 1e-3
highest = lax.Precision.HIGHEST
f32 = jnp.float32
bf16 = jnp.bfloat16

vmem = pl.BlockSpec(memory_space=pltpu.VMEM)
flops_per_micro = 1e9
vmem_limit = 24 * 1024 * 1024


def dot(a, b, dims=((1,), (0,))):
    return lax.dot_general(a, b, (dims, ((), ())), precision=highest, preferred_element_type=f32)


def dot_fast(a, b, dims=((1,), (0,))):
    return lax.dot_general(a, b, (dims, ((), ())), preferred_element_type=f32)


def gram(factor):
    return dot(factor, factor, ((0,), (0,)))


def split(x):
    high = x.astype(bf16)
    return high, (x - high.astype(f32)).astype(bf16)


def tree_sum(values):
    values = list(values)
    while len(values) > 1:
        values = [a + b for a, b in zip(values[0::2], values[1::2])]
    return values[0]


def eye_mask(n):
    return lax.broadcasted_iota(jnp.int32, (n, n), 0) == lax.broadcasted_iota(jnp.int32, (n, n), 1)


def regularized(matrix):
    n = matrix.shape[0]
    eye = eye_mask(n)
    diagonal = jnp.where(eye, matrix, 0.0)
    ridge = ridge_share * jnp.sum(diagonal) / n
    return matrix + jnp.where(eye, ridge, 0.0)


def invert(matrix, x_ref, work_ref):
    n = matrix.shape[0]
    eye = eye_mask(n)
    diagonal = jnp.where(eye, matrix, 0.0)
    by_column = lax.rsqrt(jnp.sum(diagonal, axis=0, keepdims=True))
    by_row = lax.rsqrt(jnp.sum(diagonal, axis=1, keepdims=True))
    e1 = jnp.where(eye, 0.0, -(matrix * by_column) * by_row)
    e1_half = e1.astype(bf16)
    e2 = dot_fast(e1_half, e1_half)
    e2_half = e2.astype(bf16)
    e4 = dot_fast(e2_half, e2_half)
    e4_half = e4.astype(bf16)
    part = e1 + e2 + dot_fast(e1_half, e2_half)
    part = part + e4 + dot_fast(part.astype(bf16), e4_half)
    left = jnp.sum(e4 * e4)
    x_ref[...] = (part + jnp.where(eye, 1.0, 0.0)) * by_column * by_row

    @pl.when(jnp.logical_not(left < contraction_bound))
    def _():
        work_ref[...] = jnp.where(eye, 1.0, 0.0) - e1
        lane = lax.broadcasted_iota(jnp.int32, (n, n), 1)
        sublane = lax.broadcasted_iota(jnp.int32, (n, n), 0)
        lane_row = lax.broadcasted_iota(jnp.int32, (1, n), 1)

        def step(k, carry):
            work = work_ref[...]
            row = work_ref[pl.ds(k, 1), :]
            pivot = jnp.sum(jnp.where(lane_row == k, row, 0.0), axis=1, keepdims=True)
            column = jnp.sum(jnp.where(lane == k, work, 0.0), axis=1, keepdims=True)
            inverse = 1.0 / pivot
            new_row = jnp.where(lane_row == k, inverse, row * inverse)
            others = jnp.where(lane == k, 0.0, work) - column * new_row
            work_ref[...] = jnp.where(sublane == k, new_row, others)
            return carry

        lax.fori_loop(0, n, step, 0)
        x_ref[...] = work_ref[...] * by_column * by_row


def solve(right, matrix, inverse):
    first = dot(right, inverse)
    return first + dot(right - dot(first, matrix), inverse)


def place_of(axis):
    return lax.axis_index(axis)


def at_rows(block, rows):
    return pl.ds(pl.multiple_of(block * rows, rows), rows)


def load_kernel(time_hbm, species_hbm, half_ref, time_ref, species_ref, arrived):
    half = half_ref.shape[0]
    copies = [
        pltpu.make_async_copy(time_hbm.at[at_rows(place_of("space") % 2, half)], half_ref, arrived.at[0]),
        pltpu.make_async_copy(time_hbm, time_ref, arrived.at[1]),
        pltpu.make_async_copy(species_hbm, species_ref, arrived.at[2]),
    ]
    for copy in copies:
        copy.start()
    for copy in copies:
        copy.wait()


def space_kernel(tensor_ref, time_ref, species_ref, m_a_ref, side_ref):
    species = species_ref[...]
    species_count = species.shape[0]
    time_high, time_low = split(time_ref[...])
    weights = jnp.concatenate([time_high, time_low, time_low, time_high], axis=0)
    chunk = 8
    height = chunk * species_count
    for start in range(0, tensor_ref.shape[0], height):
        high, low = split(tensor_ref[start:start + height, :])
        side = dot_fast(jnp.concatenate([high, low, high, low], axis=1), weights)
        side = side.reshape(chunk, species_count, side.shape[1])
        at = start // species_count
        side_ref[at:at + chunk] = side
        m_a_ref[at:at + chunk, :] = jnp.sum(side * species[None], axis=1)


def pack_kernel(after_ref, *refs):
    *parts, out_ref = refs
    at = 0
    for part in parts:
        out_ref[at:at + part.shape[0], :] = part[...]
        at += part.shape[0]


def peers(count, paired):
    if not paired:
        return [], list(range(1, count))
    return [(j, j + 1) for j in range(1, count - 1, 2)], [count - 1]


def place_blocks(factor_ref, place, core, own_ref, mine_ref, partner_ref, paired):
    rows = own_ref.shape[0]
    half = rows // 2
    factor_ref[at_rows(place, rows), :] = own_ref[...]
    pairs, shared = peers(factor_ref.shape[0] // rows, paired)
    for i, (first, second) in enumerate(pairs):
        step = second - first
        taken = slice(i * rows, (i + 1) * rows)
        factor_ref[at_rows(jnp.bitwise_xor(place, first + core * step), rows), :] = mine_ref[taken, :]
        factor_ref[at_rows(jnp.bitwise_xor(place, second - core * step), rows), :] = partner_ref[taken, :]
    for i, step in enumerate(shared):
        start = len(pairs) * rows + i * half
        taken = slice(start, start + half)
        at = jnp.bitwise_xor(place, step) * 2
        factor_ref[at_rows(at + core, half), :] = mine_ref[taken, :]
        factor_ref[at_rows(at + 1 - core, half), :] = partner_ref[taken, :]


def sum_kernel(*refs):
    *parts, out_ref = refs
    out_ref[...] = tree_sum([part[...] for part in parts])


def time_side_kernel(species_count, first, raw_ref, tensor_ref, side_ref):
    rows = raw_ref.shape[0]
    raw_high, raw_low = split(raw_ref[...])
    weights = jnp.concatenate([raw_high, raw_high, raw_low, raw_low], axis=0)
    for p in range(side_ref.shape[0]):
        high, low = split(tensor_ref[pl.ds(first + p, rows, stride=species_count), :])
        side_ref[p] = dot_fast(jnp.concatenate([high, low, high, low], axis=0), weights, ((0,), (0,)))


def first_inverse_kernel(species_ref, own_ref, mine_ref, partner_ref,
                         c_gram_ref, matrix_ref, inverse_ref, factor_ref, work_ref):
    place_blocks(factor_ref, place_of("tm"), place_of("space") % 2, own_ref, mine_ref, partner_ref, TIME_PAIR)
    c_gram = gram(factor_ref[...])
    c_gram_ref[...] = c_gram
    matrix = regularized(gram(species_ref[...]) * c_gram)
    matrix_ref[...] = matrix
    invert(matrix, inverse_ref, work_ref)


def space_solve_kernel(matrix_ref, inverse_ref, side_ref, *refs):
    *parts, raw_ref, keep_ref, send_ref, m_b_ref = refs
    core = place_of("space") % 2
    m_a = tree_sum([part[...] for part in parts])
    raw = solve(m_a, matrix_ref[...], inverse_ref[...])
    raw_ref[...] = raw
    rows = raw.shape[0]
    send_ref[:rows, :] = raw
    total = jnp.zeros(m_b_ref.shape, f32)
    for s in range(rows):
        total = total + side_ref[s] * raw_ref[pl.ds(s, 1), :]
    m_b_ref[...] = total
    half = keep_ref.shape[0]
    if MB_HALF:
        keep_ref[...] = m_b_ref[at_rows(core, half), :]
        send_ref[rows:, :] = m_b_ref[at_rows(1 - core, half), :]
    else:
        keep_ref[...] = total
        send_ref[rows:, :] = total


def chip_kernel(raw_ref, keep_ref, received_ref, block_ref, m_b_ref):
    core = place_of("space") % 2
    rows = raw_ref.shape[0]
    block_ref[at_rows(core, rows), :] = raw_ref[...]
    block_ref[at_rows(1 - core, rows), :] = received_ref[:rows, :]
    m_b_ref[...] = keep_ref[...] + received_ref[rows:, :]


def space_gram_kernel(c_gram_ref, own_ref, mine_ref, partner_ref,
                      a_gram_ref, matrix_ref, scale_ref, out_ref, factor_ref):
    place = place_of("space")
    place_blocks(factor_ref, place // 2, place % 2, own_ref, mine_ref, partner_ref, RAW_PAIR)
    raw_gram = gram(factor_ref[...])
    eye = eye_mask(raw_gram.shape[0])
    diagonal = jnp.where(eye, raw_gram, 0.0)
    total_rows = factor_ref.shape[0]
    by_column = lax.rsqrt(jnp.sum(diagonal, axis=0, keepdims=True) / total_rows + epsilon)
    by_row = lax.rsqrt(jnp.sum(diagonal, axis=1, keepdims=True) / total_rows + epsilon)
    scale_ref[...] = jnp.broadcast_to(by_column, scale_ref.shape)
    out_ref[...] = own_ref[at_rows(place % 2, out_ref.shape[0]), :] * by_column
    a_gram = raw_gram * by_column * by_row
    a_gram_ref[...] = a_gram
    matrix_ref[...] = regularized(a_gram * c_gram_ref[...])


def inverse_kernel(matrix_ref, inverse_ref, work_ref):
    invert(matrix_ref[...], inverse_ref, work_ref)


def refined_inverse_kernel(matrix_ref, inverse_ref, work_ref):
    matrix = matrix_ref[...]
    invert(matrix, inverse_ref, work_ref)
    inverse = inverse_ref[...]
    left = jnp.where(eye_mask(matrix.shape[0]), 1.0, 0.0) - dot(matrix, inverse)
    inverse_ref[...] = inverse + dot(inverse, left)


def species_kernel(scale_ref, matrix_ref, inverse_ref, side_ref, rest_ref, *refs):
    *parts, species_ref, scaled_ref, send_ref = refs
    core = place_of("space") % 2
    scale = scale_ref[0:1, :]
    if MB_HALF:
        mine_ref, partner_ref = parts
        half = mine_ref.shape[0]
        scaled_ref[at_rows(core, half), :] = mine_ref[...]
        scaled_ref[at_rows(1 - core, half), :] = partner_ref[...]
        m_b = scaled_ref[...] * scale
    else:
        m_b = tree_sum([part[...] for part in parts]) * scale
    raw = solve(m_b, matrix_ref[...], inverse_ref[...])
    species = raw * lax.rsqrt(jnp.mean(raw * raw, axis=0, keepdims=True) + epsilon)
    species_ref[...] = species
    scaled_ref[...] = species * scale
    time_half(1 - core, (side_ref, rest_ref), scaled_ref, send_ref)


def time_half(block, side_refs, scaled_ref, out_ref):
    half = out_ref.shape[0]
    total = jnp.zeros(out_ref.shape, f32)
    at = 0
    for side_ref in side_refs:
        for p in range(side_ref.shape[0]):
            total = total + side_ref[p, at_rows(block, half), :] * scaled_ref[at:at + 1, :]
            at += 1
    out_ref[...] = total


def time_half_kernel(side_ref, rest_ref, scaled_ref, out_ref):
    time_half(place_of("space") % 2, (side_ref, rest_ref), scaled_ref, out_ref)


def species_gram_kernel(a_gram_ref, species_ref, matrix_ref):
    matrix_ref[...] = regularized(a_gram_ref[...] * gram(species_ref[...]))


def time_solve_kernel(inverse_ref, mine_ref, partner_ref, raw_ref, squares_ref, m_c_ref):
    core = place_of("space") % 2
    half = mine_ref.shape[0]
    m_c_ref[at_rows(core, half), :] = mine_ref[...]
    m_c_ref[at_rows(1 - core, half), :] = partner_ref[...]
    raw = dot(m_c_ref[...], inverse_ref[...])
    raw_ref[...] = raw
    squares_ref[...] = jnp.broadcast_to(jnp.sum(raw * raw, axis=0, keepdims=True), squares_ref.shape)


def time_scale_kernel(total_steps, raw_ref, *refs):
    *parts, out_ref = refs
    squares = tree_sum([part[0:1, :] for part in parts])
    out_ref[...] = raw_ref[...] * lax.rsqrt(squares / total_steps + epsilon)


def exchange(value, axis, step, count):
    return lax.ppermute(value, axis, [(i, i ^ step) for i in range(count)])


def run(kernel, outs, micros, scratch=()):
    call = pl.pallas_call(
        kernel,
        out_shape=outs,
        out_specs=[vmem] * len(outs),
        scratch_shapes=list(scratch),
        cost_estimate=pl.CostEstimate(flops=int(micros * flops_per_micro), bytes_accessed=0, transcendentals=0),
        compiler_params=pltpu.CompilerParams(vmem_limit_bytes=vmem_limit),
    )

    def placed(*operands):
        return call(*[pltpu.with_memory_space_constraint(x, pltpu.VMEM) for x in operands])

    return placed


def on_device(tensor, species_factor, time_factor):
    row_count, species_count, step_count = tensor.shape
    rank = species_factor.shape[1]
    devices = lax.axis_size("space")
    blocks = lax.axis_size("tm")
    chips = devices // 2
    total_rows = row_count * devices
    total_steps = step_count * blocks

    def local(*dims):
        return pltpu.VMEM(dims, f32)

    def result(*dims):
        return jax.ShapeDtypeStruct(dims, f32)

    square = local(rank, rank)

    def over_time(value):
        return [value] + [exchange(value, "tm", j, blocks) for j in range(1, blocks)]

    def over_chips(value):
        return [value] + [exchange(value, "space", 2 * j, devices) for j in range(1, chips)]

    def to_partner(value):
        return exchange(value, "space", 1, devices)

    def block_from(block, half, axis):
        pairs, shared = peers(blocks, TIME_PAIR) if axis == "tm" else peers(chips, RAW_PAIR)
        received = []
        for steps in pairs:
            if axis == "tm":
                turns = [
                    (s * blocks + t, s * blocks + (t ^ steps[s % 2])) for s in range(devices) for t in range(blocks)
                ]
                received.append(lax.ppermute(block, ("space", "tm"), turns))
            else:
                turns = [(s, s ^ (2 * steps[s % 2])) for s in range(devices)]
                received.append(lax.ppermute(block, "space", turns))
        for j in shared:
            step, count = (j, blocks) if axis == "tm" else (2 * j, devices)
            received.append(exchange(half, axis, step, count))
        return received

    def pack(after, parts):
        return run(pack_kernel, [local(sum(part.shape[0] for part in parts), rank)], 0.3)(after, *parts)[0]

    def add(parts):
        return run(sum_kernel, [local(*parts[0].shape)], 0.3)(*parts)[0]

    half_steps = step_count // 2
    half_species = species_count // 2 if MB_HALF else species_count

    outside = pl.BlockSpec(memory_space=pltpu.HBM)
    time_half, time_here, species_here = pl.pallas_call(
        load_kernel,
        in_specs=[outside] * 2,
        out_specs=[vmem] * 3,
        out_shape=[local(half_steps, rank), local(step_count, rank), local(species_count, rank)],
        scratch_shapes=[pltpu.SemaphoreType.DMA((3,))],
        cost_estimate=pl.CostEstimate(flops=int(10 * flops_per_micro), bytes_accessed=10**8, transcendentals=0),
        compiler_params=pltpu.CompilerParams(vmem_limit_bytes=vmem_limit),
        name="load_factors",
    )(*[pltpu.with_memory_space_constraint(x, pltpu.HBM) for x in (time_factor, species_factor)])
    received = block_from(time_factor, time_half, "tm")
    m_a, side = run(
        space_kernel, [local(row_count, rank), local(row_count, species_count, rank)], 2
    )(tensor.reshape(row_count * species_count, step_count), time_here, species_here)
    m_a_parts = over_time(m_a)

    mine = pack(m_a, received)
    partner = to_partner(mine)
    c_gram, matrix, inverse = run(
        first_inverse_kernel, [square] * 3, 2, [local(total_steps, rank), square]
    )(species_here, time_here, mine, partner)

    raw, keep, send = run(
        space_solve_kernel,
        [local(row_count, rank), local(half_species, rank), local(row_count + half_species, rank)],
        1,
        [local(species_count, rank)],
    )(matrix, inverse, side, *m_a_parts)
    received = to_partner(send)
    time_sides = []
    for first, count in (
        (0, EARLY * species_count // 8), (EARLY * species_count // 8, species_count - EARLY * species_count // 8)
    ):
        time_sides += run(
            lambda *refs, first=first: time_side_kernel(species_count, first, *refs),
            [local(count, step_count, rank)],
            2 * count / species_count,
        )(raw, tensor.reshape(row_count * species_count, step_count))
    chip_block, m_b = run(chip_kernel, [local(2 * row_count, rank), local(half_species, rank)], 0.3)(
        raw, keep, received
    )
    if not MB_TREE:
        m_b = add(over_time(m_b))
    step = 1
    while MB_TREE and step < blocks:
        m_b = add([m_b, exchange(m_b, "tm", step, blocks)])
        step *= 2
    raw_blocks = block_from(chip_block, raw, "space")
    m_b_parts = over_chips(m_b)
    mine = pack(m_b, raw_blocks)
    partner = to_partner(mine)
    if MB_HALF:
        m_b = add(m_b_parts)
        m_b_parts = [m_b, to_partner(m_b)]
    a_gram, matrix, scale, space_out = run(
        space_gram_kernel, [square, square, local(8, rank), local(row_count, rank)], 1.5, [local(total_rows, rank)]
    )(c_gram, chip_block, mine, partner)
    (inverse,) = run(inverse_kernel, [square], 1, [square])(matrix)

    species, scaled, m_c_send = run(
        species_kernel, [local(species_count, rank), local(species_count, rank), local(half_steps, rank)], 1.5
    )(scale, matrix, inverse, *time_sides, *m_b_parts)

    m_c_received = to_partner(m_c_send)
    (m_c_keep,) = run(time_half_kernel, [local(half_steps, rank)], 1)(*time_sides, scaled)
    (matrix,) = run(species_gram_kernel, [square], 0.5)(a_gram, species)
    m_c_parts = over_chips(add([m_c_keep, m_c_received]))
    (inverse,) = run(refined_inverse_kernel, [square], 1, [square])(matrix)
    m_c = add(m_c_parts)
    m_c_partner = to_partner(m_c)
    raw_time, squares = run(
        time_solve_kernel, [local(step_count, rank), local(8, rank)], 1, [local(step_count, rank)]
    )(inverse, m_c, m_c_partner)

    squares = over_time(squares)
    (time_out,) = run(
        lambda *refs: time_scale_kernel(total_steps, *refs), [result(step_count, rank)], 0.5
    )(raw_time, *squares)
    return (space_out, species, time_out)


def solution(mesh):
    placed = (P("space", None, "tm"), P(), P("tm", None))
    return jax.shard_map(
        on_device,
        mesh=mesh,
        in_specs=placed,
        out_specs=(P("space", None), P(), P("tm", None)),
        check_vma=False,
    )
```

```python
import jax
import jax.numpy as jnp
from jax import lax
from jax.experimental import pallas as pl
from jax.experimental.pallas import tpu as pltpu
from jax.sharding import PartitionSpec as P


ridge_share = 0.1
epsilon = 1e-06
contraction_bound = 1e-3
highest = lax.Precision.HIGHEST
f32 = jnp.float32
bf16 = jnp.bfloat16

vmem = pl.BlockSpec(memory_space=pltpu.VMEM)
flops_per_micro = 1e9
vmem_limit = 24 * 1024 * 1024


def dot(a, b, dims=((1,), (0,))):
    return lax.dot_general(a, b, (dims, ((), ())), precision=highest, preferred_element_type=f32)


def dot_fast(a, b, dims=((1,), (0,))):
    return lax.dot_general(a, b, (dims, ((), ())), preferred_element_type=f32)


def gram(factor):
    return dot(factor, factor, ((0,), (0,)))


def split(x):
    high = x.astype(bf16)
    return high, (x - high.astype(f32)).astype(bf16)


def tree_sum(values):
    values = list(values)
    while len(values) > 1:
        values = [a + b for a, b in zip(values[0::2], values[1::2])]
    return values[0]


def eye_mask(n):
    return lax.broadcasted_iota(jnp.int32, (n, n), 0) == lax.broadcasted_iota(jnp.int32, (n, n), 1)


def regularized(matrix):
    n = matrix.shape[0]
    eye = eye_mask(n)
    diagonal = jnp.where(eye, matrix, 0.0)
    ridge = ridge_share * jnp.sum(diagonal) / n
    return matrix + jnp.where(eye, ridge, 0.0)


def invert(matrix, x_ref, work_ref):
    n = matrix.shape[0]
    eye = eye_mask(n)
    diagonal = jnp.where(eye, matrix, 0.0)
    by_column = lax.rsqrt(jnp.sum(diagonal, axis=0, keepdims=True))
    by_row = lax.rsqrt(jnp.sum(diagonal, axis=1, keepdims=True))
    e1 = jnp.where(eye, 0.0, -(matrix * by_column) * by_row)
    e1_half = e1.astype(bf16)
    e2 = dot_fast(e1_half, e1_half)
    e2_half = e2.astype(bf16)
    e4 = dot_fast(e2_half, e2_half)
    e4_half = e4.astype(bf16)
    part = e1 + e2 + dot_fast(e1_half, e2_half)
    part = part + e4 + dot_fast(part.astype(bf16), e4_half)
    left = jnp.sum(e4 * e4)
    x_ref[...] = (part + jnp.where(eye, 1.0, 0.0)) * by_column * by_row

    @pl.when(jnp.logical_not(left < contraction_bound))
    def _():
        work_ref[...] = jnp.where(eye, 1.0, 0.0) - e1
        lane = lax.broadcasted_iota(jnp.int32, (n, n), 1)
        sublane = lax.broadcasted_iota(jnp.int32, (n, n), 0)
        lane_row = lax.broadcasted_iota(jnp.int32, (1, n), 1)

        def step(k, carry):
            work = work_ref[...]
            row = work_ref[pl.ds(k, 1), :]
            pivot = jnp.sum(jnp.where(lane_row == k, row, 0.0), axis=1, keepdims=True)
            column = jnp.sum(jnp.where(lane == k, work, 0.0), axis=1, keepdims=True)
            inverse = 1.0 / pivot
            new_row = jnp.where(lane_row == k, inverse, row * inverse)
            others = jnp.where(lane == k, 0.0, work) - column * new_row
            work_ref[...] = jnp.where(sublane == k, new_row, others)
            return carry

        lax.fori_loop(0, n, step, 0)
        x_ref[...] = work_ref[...] * by_column * by_row


def solve(right, matrix, inverse):
    first = dot(right, inverse)
    return first + dot(right - dot(first, matrix), inverse)


def place_of(axis):
    return lax.axis_index(axis)


def at_rows(block, rows):
    return pl.ds(pl.multiple_of(block * rows, rows), rows)


def load_kernel(time_hbm, species_hbm, half_ref, time_ref, species_ref, arrived):
    half = half_ref.shape[0]
    copies = [
        pltpu.make_async_copy(time_hbm.at[at_rows(place_of("space") % 2, half)], half_ref, arrived.at[0]),
        pltpu.make_async_copy(time_hbm, time_ref, arrived.at[1]),
        pltpu.make_async_copy(species_hbm, species_ref, arrived.at[2]),
    ]
    for copy in copies:
        copy.start()
    for copy in copies:
        copy.wait()


def space_kernel(tensor_ref, time_ref, species_ref, m_a_ref, side_ref):
    species = species_ref[...]
    species_count = species.shape[0]
    time_high, time_low = split(time_ref[...])
    weights = jnp.concatenate([time_high, time_low, time_low, time_high], axis=0)
    chunk = 8
    height = chunk * species_count
    for start in range(0, tensor_ref.shape[0], height):
        high, low = split(tensor_ref[start:start + height, :])
        side = dot_fast(jnp.concatenate([high, low, high, low], axis=1), weights)
        side = side.reshape(chunk, species_count, side.shape[1])
        at = start // species_count
        side_ref[at:at + chunk] = side
        m_a_ref[at:at + chunk, :] = jnp.sum(side * species[None], axis=1)


def pack_kernel(after_ref, *refs):
    *parts, out_ref = refs
    at = 0
    for part in parts:
        out_ref[at:at + part.shape[0], :] = part[...]
        at += part.shape[0]


def peers(count):
    return [(j, j + 1) for j in range(1, count - 1, 2)], count - 1


def place_blocks(factor_ref, place, core, own_ref, mine_ref, partner_ref):
    rows = own_ref.shape[0]
    half = rows // 2
    factor_ref[at_rows(place, rows), :] = own_ref[...]
    pairs, last = peers(factor_ref.shape[0] // rows)
    for i, (first, second) in enumerate(pairs):
        step = second - first
        taken = slice(i * rows, (i + 1) * rows)
        factor_ref[at_rows(jnp.bitwise_xor(place, first + core * step), rows), :] = mine_ref[taken, :]
        factor_ref[at_rows(jnp.bitwise_xor(place, second - core * step), rows), :] = partner_ref[taken, :]
    taken = slice(len(pairs) * rows, len(pairs) * rows + half)
    at = jnp.bitwise_xor(place, last) * 2
    factor_ref[at_rows(at + core, half), :] = mine_ref[taken, :]
    factor_ref[at_rows(at + 1 - core, half), :] = partner_ref[taken, :]


def sum_kernel(*refs):
    *parts, out_ref = refs
    out_ref[...] = tree_sum([part[...] for part in parts])


def time_side_kernel(species_count, first, raw_ref, tensor_ref, side_ref):
    rows = raw_ref.shape[0]
    raw_high, raw_low = split(raw_ref[...])
    weights = jnp.concatenate([raw_high, raw_high, raw_low, raw_low], axis=0)
    for p in range(side_ref.shape[0]):
        high, low = split(tensor_ref[pl.ds(first + p, rows, stride=species_count), :])
        side_ref[p] = dot_fast(jnp.concatenate([high, low, high, low], axis=0), weights, ((0,), (0,)))


def first_inverse_kernel(species_ref, own_ref, mine_ref, partner_ref,
                         c_gram_ref, matrix_ref, inverse_ref, factor_ref, work_ref):
    place_blocks(factor_ref, place_of("tm"), place_of("space") % 2, own_ref, mine_ref, partner_ref)
    c_gram = gram(factor_ref[...])
    c_gram_ref[...] = c_gram
    matrix = regularized(gram(species_ref[...]) * c_gram)
    matrix_ref[...] = matrix
    invert(matrix, inverse_ref, work_ref)


def space_solve_kernel(matrix_ref, inverse_ref, side_ref, *refs):
    *parts, raw_ref, keep_ref, send_ref, m_b_ref = refs
    core = place_of("space") % 2
    m_a = tree_sum([part[...] for part in parts])
    raw = solve(m_a, matrix_ref[...], inverse_ref[...])
    raw_ref[...] = raw
    rows = raw.shape[0]
    send_ref[:rows, :] = raw
    total = jnp.zeros(m_b_ref.shape, f32)
    for s in range(rows):
        total = total + side_ref[s] * raw_ref[pl.ds(s, 1), :]
    m_b_ref[...] = total
    half = keep_ref.shape[0]
    keep_ref[...] = m_b_ref[at_rows(core, half), :]
    send_ref[rows:, :] = m_b_ref[at_rows(1 - core, half), :]


def chip_kernel(raw_ref, keep_ref, received_ref, block_ref, m_b_ref):
    core = place_of("space") % 2
    rows = raw_ref.shape[0]
    block_ref[at_rows(core, rows), :] = raw_ref[...]
    block_ref[at_rows(1 - core, rows), :] = received_ref[:rows, :]
    m_b_ref[...] = keep_ref[...] + received_ref[rows:, :]


def space_gram_kernel(c_gram_ref, own_ref, mine_ref, partner_ref,
                      a_gram_ref, matrix_ref, scale_ref, out_ref, factor_ref):
    place = place_of("space")
    place_blocks(factor_ref, place // 2, place % 2, own_ref, mine_ref, partner_ref)
    raw_gram = gram(factor_ref[...])
    eye = eye_mask(raw_gram.shape[0])
    diagonal = jnp.where(eye, raw_gram, 0.0)
    total_rows = factor_ref.shape[0]
    by_column = lax.rsqrt(jnp.sum(diagonal, axis=0, keepdims=True) / total_rows + epsilon)
    by_row = lax.rsqrt(jnp.sum(diagonal, axis=1, keepdims=True) / total_rows + epsilon)
    scale_ref[...] = jnp.broadcast_to(by_column, scale_ref.shape)
    out_ref[...] = own_ref[at_rows(place % 2, out_ref.shape[0]), :] * by_column
    a_gram = raw_gram * by_column * by_row
    a_gram_ref[...] = a_gram
    matrix_ref[...] = regularized(a_gram * c_gram_ref[...])


def inverse_kernel(matrix_ref, inverse_ref, work_ref):
    invert(matrix_ref[...], inverse_ref, work_ref)


def refined_inverse_kernel(matrix_ref, inverse_ref, work_ref):
    matrix = matrix_ref[...]
    invert(matrix, inverse_ref, work_ref)
    inverse = inverse_ref[...]
    left = jnp.where(eye_mask(matrix.shape[0]), 1.0, 0.0) - dot(matrix, inverse)
    inverse_ref[...] = inverse + dot(inverse, left)


def species_kernel(scale_ref, matrix_ref, inverse_ref, side_ref, rest_ref, mine_ref, partner_ref,
                   species_ref, scaled_ref, send_ref):
    core = place_of("space") % 2
    scale = scale_ref[0:1, :]
    half = mine_ref.shape[0]
    scaled_ref[at_rows(core, half), :] = mine_ref[...]
    scaled_ref[at_rows(1 - core, half), :] = partner_ref[...]
    m_b = scaled_ref[...] * scale
    raw = solve(m_b, matrix_ref[...], inverse_ref[...])
    species = raw * lax.rsqrt(jnp.mean(raw * raw, axis=0, keepdims=True) + epsilon)
    species_ref[...] = species
    scaled_ref[...] = species * scale
    time_half(1 - core, (side_ref, rest_ref), scaled_ref, send_ref)


def time_half(block, side_refs, scaled_ref, out_ref):
    half = out_ref.shape[0]
    total = jnp.zeros(out_ref.shape, f32)
    at = 0
    for side_ref in side_refs:
        for p in range(side_ref.shape[0]):
            total = total + side_ref[p, at_rows(block, half), :] * scaled_ref[at:at + 1, :]
            at += 1
    out_ref[...] = total


def time_half_kernel(side_ref, rest_ref, scaled_ref, out_ref):
    time_half(place_of("space") % 2, (side_ref, rest_ref), scaled_ref, out_ref)


def species_gram_kernel(a_gram_ref, species_ref, matrix_ref):
    matrix_ref[...] = regularized(a_gram_ref[...] * gram(species_ref[...]))


def time_solve_kernel(inverse_ref, mine_ref, partner_ref, raw_ref, squares_ref, m_c_ref):
    core = place_of("space") % 2
    half = mine_ref.shape[0]
    m_c_ref[at_rows(core, half), :] = mine_ref[...]
    m_c_ref[at_rows(1 - core, half), :] = partner_ref[...]
    raw = dot(m_c_ref[...], inverse_ref[...])
    raw_ref[...] = raw
    squares_ref[...] = jnp.broadcast_to(jnp.sum(raw * raw, axis=0, keepdims=True), squares_ref.shape)


def time_scale_kernel(total_steps, raw_ref, *refs):
    *parts, out_ref = refs
    squares = tree_sum([part[0:1, :] for part in parts])
    out_ref[...] = raw_ref[...] * lax.rsqrt(squares / total_steps + epsilon)


def exchange(value, axis, step, count):
    return lax.ppermute(value, axis, [(i, i ^ step) for i in range(count)])


def run(kernel, outs, micros, scratch=()):
    call = pl.pallas_call(
        kernel,
        out_shape=outs,
        out_specs=[vmem] * len(outs),
        scratch_shapes=list(scratch),
        cost_estimate=pl.CostEstimate(flops=int(micros * flops_per_micro), bytes_accessed=0, transcendentals=0),
        compiler_params=pltpu.CompilerParams(vmem_limit_bytes=vmem_limit),
    )

    def placed(*operands):
        return call(*[pltpu.with_memory_space_constraint(x, pltpu.VMEM) for x in operands])

    return placed


def on_device(tensor, species_factor, time_factor):
    row_count, species_count, step_count = tensor.shape
    rank = species_factor.shape[1]
    devices = lax.axis_size("space")
    blocks = lax.axis_size("tm")
    chips = devices // 2
    total_rows = row_count * devices
    total_steps = step_count * blocks

    def local(*dims):
        return pltpu.VMEM(dims, f32)

    def result(*dims):
        return jax.ShapeDtypeStruct(dims, f32)

    square = local(rank, rank)

    def over_time(value):
        return [value] + [exchange(value, "tm", j, blocks) for j in range(1, blocks)]

    def over_chips(value):
        return [value] + [exchange(value, "space", 2 * j, devices) for j in range(1, chips)]

    def to_partner(value):
        return exchange(value, "space", 1, devices)

    def block_from(block, half, axis):
        pairs, last = peers(blocks if axis == "tm" else chips)
        received = []
        for steps in pairs:
            if axis == "tm":
                turns = [
                    (s * blocks + t, s * blocks + (t ^ steps[s % 2])) for s in range(devices) for t in range(blocks)
                ]
                received.append(lax.ppermute(block, ("space", "tm"), turns))
            else:
                turns = [(s, s ^ (2 * steps[s % 2])) for s in range(devices)]
                received.append(lax.ppermute(block, "space", turns))
        step, count = (last, blocks) if axis == "tm" else (2 * last, devices)
        return received + [exchange(half, axis, step, count)]

    def pack(after, parts):
        return run(pack_kernel, [local(sum(part.shape[0] for part in parts), rank)], 0.3)(after, *parts)[0]

    def add(parts):
        return run(sum_kernel, [local(*parts[0].shape)], 0.3)(*parts)[0]

    half_steps = step_count // 2
    half_species = species_count // 2

    outside = pl.BlockSpec(memory_space=pltpu.HBM)
    time_half, time_here, species_here = pl.pallas_call(
        load_kernel,
        in_specs=[outside] * 2,
        out_specs=[vmem] * 3,
        out_shape=[local(half_steps, rank), local(step_count, rank), local(species_count, rank)],
        scratch_shapes=[pltpu.SemaphoreType.DMA((3,))],
        cost_estimate=pl.CostEstimate(flops=int(10 * flops_per_micro), bytes_accessed=10**8, transcendentals=0),
        compiler_params=pltpu.CompilerParams(vmem_limit_bytes=vmem_limit),
        name="load",
    )(*[pltpu.with_memory_space_constraint(x, pltpu.HBM) for x in (time_factor, species_factor)])
    received = block_from(time_factor, time_half, "tm")
    m_a, side = run(
        space_kernel, [local(row_count, rank), local(row_count, species_count, rank)], 2
    )(tensor.reshape(row_count * species_count, step_count), time_here, species_here)
    m_a_parts = over_time(m_a)

    mine = pack(m_a, received)
    partner = to_partner(mine)
    c_gram, matrix, inverse = run(
        first_inverse_kernel, [square] * 3, 2, [local(total_steps, rank), square]
    )(species_here, time_here, mine, partner)

    raw, keep, send = run(
        space_solve_kernel,
        [local(row_count, rank), local(half_species, rank), local(row_count + half_species, rank)],
        1,
        [local(species_count, rank)],
    )(matrix, inverse, side, *m_a_parts)
    received = to_partner(send)
    early = 5 * species_count // 8
    time_sides = []
    for first, count in ((0, early), (early, species_count - early)):
        time_sides += run(
            lambda *refs, first=first: time_side_kernel(species_count, first, *refs),
            [local(count, step_count, rank)],
            2 * count / species_count,
        )(raw, tensor.reshape(row_count * species_count, step_count))
    chip_block, m_b = run(chip_kernel, [local(2 * row_count, rank), local(half_species, rank)], 0.3)(
        raw, keep, received
    )
    m_b = add(over_time(m_b))
    raw_blocks = block_from(chip_block, raw, "space")
    m_b_parts = over_chips(m_b)
    mine = pack(m_b, raw_blocks)
    partner = to_partner(mine)
    m_b = add(m_b_parts)
    m_b_partner = to_partner(m_b)
    a_gram, matrix, scale, space_out = run(
        space_gram_kernel, [square, square, local(8, rank), local(row_count, rank)], 1.5, [local(total_rows, rank)]
    )(c_gram, chip_block, mine, partner)
    (inverse,) = run(inverse_kernel, [square], 1, [square])(matrix)

    species, scaled, m_c_send = run(
        species_kernel, [local(species_count, rank), local(species_count, rank), local(half_steps, rank)], 1.5
    )(scale, matrix, inverse, *time_sides, m_b, m_b_partner)

    m_c_received = to_partner(m_c_send)
    (m_c_keep,) = run(time_half_kernel, [local(half_steps, rank)], 1)(*time_sides, scaled)
    (matrix,) = run(species_gram_kernel, [square], 0.5)(a_gram, species)
    m_c_parts = over_chips(add([m_c_keep, m_c_received]))
    (inverse,) = run(refined_inverse_kernel, [square], 1, [square])(matrix)
    m_c = add(m_c_parts)
    m_c_partner = to_partner(m_c)
    raw_time, squares = run(
        time_solve_kernel, [local(step_count, rank), local(8, rank)], 1, [local(step_count, rank)]
    )(inverse, m_c, m_c_partner)

    squares = over_time(squares)
    (time_out,) = run(
        lambda *refs: time_scale_kernel(total_steps, *refs), [result(step_count, rank)], 0.5
    )(raw_time, *squares)
    return (space_out, species, time_out)


def solution(mesh):
    placed = (P("space", None, "tm"), P(), P("tm", None))
    return jax.shard_map(
        on_device,
        mesh=mesh,
        in_specs=placed,
        out_specs=(P("space", None), P(), P("tm", None)),
        check_vma=False,
    )
```

```python
import jax
import jax.numpy as jnp
from jax import lax
from jax.experimental import pallas as pl
from jax.experimental.pallas import tpu as pltpu
from jax.sharding import PartitionSpec as P


ridge_share = 0.1
epsilon = 1e-06
contraction_bound = 1e-3
f32 = jnp.float32
bf16 = jnp.bfloat16

vmem = pl.BlockSpec(memory_space=pltpu.VMEM)
flops_per_micro = 1e9
vmem_limit = 24 * 1024 * 1024


def split3(x):
    high = x.astype(bf16)
    rest = x - high.astype(f32)
    middle = rest.astype(bf16)
    return high, middle, (rest - middle.astype(f32)).astype(bf16)


def dot(a, b):
    rows = a.shape[0]
    high, middle, low = split3(a)
    b_high, b_middle, b_low = split3(b)
    two = jnp.concatenate([high, middle], axis=0)
    first = dot_fast(jnp.concatenate([two, low], axis=0), b_high)
    second = dot_fast(two, b_middle)
    small = first[2 * rows:] + second[rows:] + dot_fast(high, b_low)
    return first[:rows] + (first[rows:2 * rows] + second[:rows] + small)


def dot_fast(a, b, dims=((1,), (0,))):
    return lax.dot_general(a, b, (dims, ((), ())), preferred_element_type=f32)


def gram(factor):
    n = factor.shape[1]
    rows_first = ((0,), (0,))
    high, middle, low = split3(factor)
    products = dot_fast(high, jnp.concatenate([high, middle, low], axis=1), rows_first)
    mixed = products[:, n:2 * n] + products[:, 2 * n:]
    return products[:, :n] + (mixed + mixed.T + dot_fast(middle, middle, rows_first))


def split(x):
    high = x.astype(bf16)
    return high, (x - high.astype(f32)).astype(bf16)


def tree_sum(values):
    values = list(values)
    while len(values) > 1:
        values = [a + b for a, b in zip(values[0::2], values[1::2])]
    return values[0]


def eye_mask(n):
    return lax.broadcasted_iota(jnp.int32, (n, n), 0) == lax.broadcasted_iota(jnp.int32, (n, n), 1)


def regularized(matrix):
    n = matrix.shape[0]
    eye = eye_mask(n)
    diagonal = jnp.where(eye, matrix, 0.0)
    ridge = ridge_share * jnp.sum(diagonal) / n
    return matrix + jnp.where(eye, ridge, 0.0)


def invert(matrix, x_ref, work_ref):
    n = matrix.shape[0]
    eye = eye_mask(n)
    diagonal = jnp.where(eye, matrix, 0.0)
    by_column = lax.rsqrt(jnp.sum(diagonal, axis=0, keepdims=True))
    by_row = lax.rsqrt(jnp.sum(diagonal, axis=1, keepdims=True))
    e1 = jnp.where(eye, 0.0, -(matrix * by_column) * by_row)
    e1_half = e1.astype(bf16)
    e2 = dot_fast(e1_half, e1_half)
    e2_half = e2.astype(bf16)
    e4 = dot_fast(e2_half, e2_half)
    e4_half = e4.astype(bf16)
    part = e1 + e2 + dot_fast(e1_half, e2_half)
    part = part + e4 + dot_fast(part.astype(bf16), e4_half)
    left = jnp.sum(e4 * e4)
    x_ref[...] = (part + jnp.where(eye, 1.0, 0.0)) * by_column * by_row

    @pl.when(jnp.logical_not(left < contraction_bound))
    def _():
        work_ref[...] = jnp.where(eye, 1.0, 0.0) - e1
        lane = lax.broadcasted_iota(jnp.int32, (n, n), 1)
        sublane = lax.broadcasted_iota(jnp.int32, (n, n), 0)
        lane_row = lax.broadcasted_iota(jnp.int32, (1, n), 1)

        def step(k, carry):
            work = work_ref[...]
            row = work_ref[pl.ds(k, 1), :]
            pivot = jnp.sum(jnp.where(lane_row == k, row, 0.0), axis=1, keepdims=True)
            column = jnp.sum(jnp.where(lane == k, work, 0.0), axis=1, keepdims=True)
            inverse = 1.0 / pivot
            new_row = jnp.where(lane_row == k, inverse, row * inverse)
            others = jnp.where(lane == k, 0.0, work) - column * new_row
            work_ref[...] = jnp.where(sublane == k, new_row, others)
            return carry

        lax.fori_loop(0, n, step, 0)
        x_ref[...] = work_ref[...] * by_column * by_row


def solve(right, matrix, inverse):
    first = dot(right, inverse)
    return first + dot(right - dot(first, matrix), inverse)


def place_of(axis):
    return lax.axis_index(axis)


def at_rows(block, rows):
    return pl.ds(pl.multiple_of(block * rows, rows), rows)


def load_kernel(time_hbm, species_hbm, half_ref, time_ref, species_ref, arrived):
    half = half_ref.shape[0]
    copies = [
        pltpu.make_async_copy(time_hbm.at[at_rows(place_of("space") % 2, half)], half_ref, arrived.at[0]),
        pltpu.make_async_copy(time_hbm, time_ref, arrived.at[1]),
        pltpu.make_async_copy(species_hbm, species_ref, arrived.at[2]),
    ]
    for copy in copies:
        copy.start()
    for copy in copies:
        copy.wait()


def space_kernel(tensor_ref, time_ref, species_ref, m_a_ref, side_ref):
    species = species_ref[...]
    species_count = species.shape[0]
    time_high, time_low = split(time_ref[...])
    weights = jnp.concatenate([time_high, time_low, time_low, time_high], axis=0)
    chunk = 8
    height = chunk * species_count
    for start in range(0, tensor_ref.shape[0], height):
        high, low = split(tensor_ref[start:start + height, :])
        side = dot_fast(jnp.concatenate([high, low, high, low], axis=1), weights)
        side = side.reshape(chunk, species_count, side.shape[1])
        at = start // species_count
        side_ref[at:at + chunk] = side
        m_a_ref[at:at + chunk, :] = jnp.sum(side * species[None], axis=1)


def pack_kernel(after_ref, *refs):
    *parts, out_ref = refs
    at = 0
    for part in parts:
        out_ref[at:at + part.shape[0], :] = part[...]
        at += part.shape[0]


def peers(count):
    return [(j, j + 1) for j in range(1, count - 1, 2)], count - 1


def place_blocks(factor_ref, place, core, own_ref, mine_ref, partner_ref):
    rows = own_ref.shape[0]
    half = rows // 2
    factor_ref[at_rows(place, rows), :] = own_ref[...]
    pairs, last = peers(factor_ref.shape[0] // rows)
    for i, (first, second) in enumerate(pairs):
        step = second - first
        taken = slice(i * rows, (i + 1) * rows)
        factor_ref[at_rows(jnp.bitwise_xor(place, first + core * step), rows), :] = mine_ref[taken, :]
        factor_ref[at_rows(jnp.bitwise_xor(place, second - core * step), rows), :] = partner_ref[taken, :]
    taken = slice(len(pairs) * rows, len(pairs) * rows + half)
    at = jnp.bitwise_xor(place, last) * 2
    factor_ref[at_rows(at + core, half), :] = mine_ref[taken, :]
    factor_ref[at_rows(at + 1 - core, half), :] = partner_ref[taken, :]


def sum_kernel(*refs):
    *parts, out_ref = refs
    out_ref[...] = tree_sum([part[...] for part in parts])


def time_side_kernel(species_count, first, raw_ref, tensor_ref, side_ref):
    rows = raw_ref.shape[0]
    raw_high, raw_low = split(raw_ref[...])
    weights = jnp.concatenate([raw_high, raw_high, raw_low, raw_low], axis=0)
    for p in range(side_ref.shape[0]):
        high, low = split(tensor_ref[pl.ds(first + p, rows, stride=species_count), :])
        side_ref[p] = dot_fast(jnp.concatenate([high, low, high, low], axis=0), weights, ((0,), (0,)))


def first_inverse_kernel(species_ref, own_ref, mine_ref, partner_ref,
                         c_gram_ref, matrix_ref, inverse_ref, factor_ref, work_ref):
    place_blocks(factor_ref, place_of("tm"), place_of("space") % 2, own_ref, mine_ref, partner_ref)
    c_gram = gram(factor_ref[...])
    c_gram_ref[...] = c_gram
    matrix = regularized(gram(species_ref[...]) * c_gram)
    matrix_ref[...] = matrix
    invert(matrix, inverse_ref, work_ref)


def space_solve_kernel(matrix_ref, inverse_ref, side_ref, *refs):
    *parts, raw_ref, keep_ref, send_ref, m_b_ref = refs
    core = place_of("space") % 2
    m_a = tree_sum([part[...] for part in parts])
    raw = solve(m_a, matrix_ref[...], inverse_ref[...])
    raw_ref[...] = raw
    rows = raw.shape[0]
    send_ref[:rows, :] = raw
    total = jnp.zeros(m_b_ref.shape, f32)
    for s in range(rows):
        total = total + side_ref[s] * raw_ref[pl.ds(s, 1), :]
    m_b_ref[...] = total
    half = keep_ref.shape[0]
    keep_ref[...] = m_b_ref[at_rows(core, half), :]
    send_ref[rows:, :] = m_b_ref[at_rows(1 - core, half), :]


def chip_kernel(raw_ref, keep_ref, received_ref, block_ref, m_b_ref):
    core = place_of("space") % 2
    rows = raw_ref.shape[0]
    block_ref[at_rows(core, rows), :] = raw_ref[...]
    block_ref[at_rows(1 - core, rows), :] = received_ref[:rows, :]
    m_b_ref[...] = keep_ref[...] + received_ref[rows:, :]


def space_gram_kernel(c_gram_ref, own_ref, mine_ref, partner_ref,
                      a_gram_ref, matrix_ref, scale_ref, out_ref, factor_ref):
    place = place_of("space")
    place_blocks(factor_ref, place // 2, place % 2, own_ref, mine_ref, partner_ref)
    raw_gram = gram(factor_ref[...])
    eye = eye_mask(raw_gram.shape[0])
    diagonal = jnp.where(eye, raw_gram, 0.0)
    total_rows = factor_ref.shape[0]
    by_column = lax.rsqrt(jnp.sum(diagonal, axis=0, keepdims=True) / total_rows + epsilon)
    by_row = lax.rsqrt(jnp.sum(diagonal, axis=1, keepdims=True) / total_rows + epsilon)
    scale_ref[...] = jnp.broadcast_to(by_column, scale_ref.shape)
    out_ref[...] = own_ref[at_rows(place % 2, out_ref.shape[0]), :] * by_column
    a_gram = raw_gram * by_column * by_row
    a_gram_ref[...] = a_gram
    matrix_ref[...] = regularized(a_gram * c_gram_ref[...])


def inverse_kernel(matrix_ref, inverse_ref, work_ref):
    invert(matrix_ref[...], inverse_ref, work_ref)


def refined_inverse_kernel(matrix_ref, inverse_ref, work_ref):
    matrix = matrix_ref[...]
    invert(matrix, inverse_ref, work_ref)
    inverse = inverse_ref[...]
    left = jnp.where(eye_mask(matrix.shape[0]), 1.0, 0.0) - dot(matrix, inverse)
    inverse_ref[...] = inverse + dot(inverse, left)


def species_kernel(scale_ref, matrix_ref, inverse_ref, side_ref, rest_ref, mine_ref, partner_ref,
                   species_ref, scaled_ref, send_ref):
    core = place_of("space") % 2
    scale = scale_ref[0:1, :]
    half = mine_ref.shape[0]
    scaled_ref[at_rows(core, half), :] = mine_ref[...]
    scaled_ref[at_rows(1 - core, half), :] = partner_ref[...]
    m_b = scaled_ref[...] * scale
    raw = solve(m_b, matrix_ref[...], inverse_ref[...])
    species = raw * lax.rsqrt(jnp.mean(raw * raw, axis=0, keepdims=True) + epsilon)
    species_ref[...] = species
    scaled_ref[...] = species * scale
    time_half(1 - core, (side_ref, rest_ref), scaled_ref, send_ref)


def time_half(block, side_refs, scaled_ref, out_ref):
    half = out_ref.shape[0]
    total = jnp.zeros(out_ref.shape, f32)
    at = 0
    for side_ref in side_refs:
        for p in range(side_ref.shape[0]):
            total = total + side_ref[p, at_rows(block, half), :] * scaled_ref[at:at + 1, :]
            at += 1
    out_ref[...] = total


def time_half_kernel(side_ref, rest_ref, scaled_ref, out_ref):
    time_half(place_of("space") % 2, (side_ref, rest_ref), scaled_ref, out_ref)


def species_gram_kernel(a_gram_ref, species_ref, matrix_ref):
    matrix_ref[...] = regularized(a_gram_ref[...] * gram(species_ref[...]))


def time_solve_kernel(inverse_ref, mine_ref, partner_ref, raw_ref, squares_ref, m_c_ref):
    core = place_of("space") % 2
    half = mine_ref.shape[0]
    m_c_ref[at_rows(core, half), :] = mine_ref[...]
    m_c_ref[at_rows(1 - core, half), :] = partner_ref[...]
    raw = dot(m_c_ref[...], inverse_ref[...])
    raw_ref[...] = raw
    squares_ref[...] = jnp.broadcast_to(jnp.sum(raw * raw, axis=0, keepdims=True), squares_ref.shape)


def time_scale_kernel(total_steps, raw_ref, *refs):
    *parts, out_ref = refs
    squares = tree_sum([part[0:1, :] for part in parts])
    out_ref[...] = raw_ref[...] * lax.rsqrt(squares / total_steps + epsilon)


def exchange(value, axis, step, count):
    return lax.ppermute(value, axis, [(i, i ^ step) for i in range(count)])


def run(kernel, outs, micros, scratch=()):
    call = pl.pallas_call(
        kernel,
        out_shape=outs,
        out_specs=[vmem] * len(outs),
        scratch_shapes=list(scratch),
        cost_estimate=pl.CostEstimate(flops=int(micros * flops_per_micro), bytes_accessed=0, transcendentals=0),
        compiler_params=pltpu.CompilerParams(vmem_limit_bytes=vmem_limit),
    )

    def placed(*operands):
        return call(*[pltpu.with_memory_space_constraint(x, pltpu.VMEM) for x in operands])

    return placed


def on_device(tensor, species_factor, time_factor):
    row_count, species_count, step_count = tensor.shape
    rank = species_factor.shape[1]
    devices = lax.axis_size("space")
    blocks = lax.axis_size("tm")
    chips = devices // 2
    total_rows = row_count * devices
    total_steps = step_count * blocks

    def local(*dims):
        return pltpu.VMEM(dims, f32)

    def result(*dims):
        return jax.ShapeDtypeStruct(dims, f32)

    square = local(rank, rank)

    def over_time(value):
        return [value] + [exchange(value, "tm", j, blocks) for j in range(1, blocks)]

    def over_chips(value):
        return [value] + [exchange(value, "space", 2 * j, devices) for j in range(1, chips)]

    def to_partner(value):
        return exchange(value, "space", 1, devices)

    def block_from(block, half, axis):
        pairs, last = peers(blocks if axis == "tm" else chips)
        received = []
        for steps in pairs:
            if axis == "tm":
                turns = [
                    (s * blocks + t, s * blocks + (t ^ steps[s % 2])) for s in range(devices) for t in range(blocks)
                ]
                received.append(lax.ppermute(block, ("space", "tm"), turns))
            else:
                turns = [(s, s ^ (2 * steps[s % 2])) for s in range(devices)]
                received.append(lax.ppermute(block, "space", turns))
        step, count = (last, blocks) if axis == "tm" else (2 * last, devices)
        return received + [exchange(half, axis, step, count)]

    def pack(after, parts):
        return run(pack_kernel, [local(sum(part.shape[0] for part in parts), rank)], 0.3)(after, *parts)[0]

    def add(parts):
        return run(sum_kernel, [local(*parts[0].shape)], 0.3)(*parts)[0]

    half_steps = step_count // 2
    half_species = species_count // 2

    outside = pl.BlockSpec(memory_space=pltpu.HBM)
    time_half, time_here, species_here = pl.pallas_call(
        load_kernel,
        in_specs=[outside] * 2,
        out_specs=[vmem] * 3,
        out_shape=[local(half_steps, rank), local(step_count, rank), local(species_count, rank)],
        scratch_shapes=[pltpu.SemaphoreType.DMA((3,))],
        cost_estimate=pl.CostEstimate(flops=int(10 * flops_per_micro), bytes_accessed=10**8, transcendentals=0),
        compiler_params=pltpu.CompilerParams(vmem_limit_bytes=vmem_limit),
        name="load",
    )(*[pltpu.with_memory_space_constraint(x, pltpu.HBM) for x in (time_factor, species_factor)])
    received = block_from(time_factor, time_half, "tm")
    m_a, side = run(
        space_kernel, [local(row_count, rank), local(row_count, species_count, rank)], 2
    )(tensor.reshape(row_count * species_count, step_count), time_here, species_here)
    m_a_parts = over_time(m_a)

    mine = pack(m_a, received)
    partner = to_partner(mine)
    c_gram, matrix, inverse = run(
        first_inverse_kernel, [square] * 3, 2, [local(total_steps, rank), square]
    )(species_here, time_here, mine, partner)

    raw, keep, send = run(
        space_solve_kernel,
        [local(row_count, rank), local(half_species, rank), local(row_count + half_species, rank)],
        1,
        [local(species_count, rank)],
    )(matrix, inverse, side, *m_a_parts)
    received = to_partner(send)
    early = 5 * species_count // 8
    time_sides = []
    for first, count in ((0, early), (early, species_count - early)):
        time_sides += run(
            lambda *refs, first=first: time_side_kernel(species_count, first, *refs),
            [local(count, step_count, rank)],
            2 * count / species_count,
        )(raw, tensor.reshape(row_count * species_count, step_count))
    chip_block, m_b = run(chip_kernel, [local(2 * row_count, rank), local(half_species, rank)], 0.3)(
        raw, keep, received
    )
    m_b = add(over_time(m_b))
    raw_blocks = block_from(chip_block, raw, "space")
    m_b_parts = over_chips(m_b)
    mine = pack(m_b, raw_blocks)
    partner = to_partner(mine)
    m_b = add(m_b_parts)
    m_b_partner = to_partner(m_b)
    a_gram, matrix, scale, space_out = run(
        space_gram_kernel, [square, square, local(8, rank), local(row_count, rank)], 1.5, [local(total_rows, rank)]
    )(c_gram, chip_block, mine, partner)
    (inverse,) = run(inverse_kernel, [square], 1, [square])(matrix)

    species, scaled, m_c_send = run(
        species_kernel, [local(species_count, rank), local(species_count, rank), local(half_steps, rank)], 1.5
    )(scale, matrix, inverse, *time_sides, m_b, m_b_partner)

    m_c_received = to_partner(m_c_send)
    (m_c_keep,) = run(time_half_kernel, [local(half_steps, rank)], 1)(*time_sides, scaled)
    (matrix,) = run(species_gram_kernel, [square], 0.5)(a_gram, species)
    m_c_parts = over_chips(add([m_c_keep, m_c_received]))
    (inverse,) = run(refined_inverse_kernel, [square], 1, [square])(matrix)
    m_c = add(m_c_parts)
    m_c_partner = to_partner(m_c)
    raw_time, squares = run(
        time_solve_kernel, [local(step_count, rank), local(8, rank)], 1, [local(step_count, rank)]
    )(inverse, m_c, m_c_partner)

    squares = over_time(squares)
    (time_out,) = run(
        lambda *refs: time_scale_kernel(total_steps, *refs), [result(step_count, rank)], 0.5
    )(raw_time, *squares)
    return (space_out, species, time_out)


def solution(mesh):
    placed = (P("space", None, "tm"), P(), P("tm", None))
    return jax.shard_map(
        on_device,
        mesh=mesh,
        in_specs=placed,
        out_specs=(P("space", None), P(), P("tm", None)),
        check_vma=False,
    )
```

```python
import jax
import jax.numpy as jnp
from jax import lax
from jax.experimental import pallas as pl
from jax.experimental.pallas import tpu as pltpu
from jax.sharding import PartitionSpec as P


ridge_share = 0.1
epsilon = 1e-06
contraction_bound = 1e-3
f32 = jnp.float32
bf16 = jnp.bfloat16

vmem = pl.BlockSpec(memory_space=pltpu.VMEM)
flops_per_micro = 1e9
vmem_limit = 24 * 1024 * 1024


def split3(x):
    high = x.astype(bf16)
    rest = x - high.astype(f32)
    middle = rest.astype(bf16)
    return high, middle, (rest - middle.astype(f32)).astype(bf16)


def dot(a, b):
    rows = a.shape[0]
    high, middle, low = split3(a)
    b_high, b_middle, b_low = split3(b)
    two = jnp.concatenate([high, middle], axis=0)
    first = dot_fast(jnp.concatenate([two, low], axis=0), b_high)
    second = dot_fast(two, b_middle)
    small = first[2 * rows:] + second[rows:] + dot_fast(high, b_low)
    return first[:rows] + (first[rows:2 * rows] + second[:rows] + small)


def dot_fast(a, b, dims=((1,), (0,))):
    return lax.dot_general(a, b, (dims, ((), ())), preferred_element_type=f32)


def gram(factor):
    n = factor.shape[1]
    rows_first = ((0,), (0,))
    high, middle, low = split3(factor)
    products = dot_fast(high, jnp.concatenate([high, middle, low], axis=1), rows_first)
    mixed = products[:, n:2 * n] + products[:, 2 * n:]
    return products[:, :n] + (mixed + mixed.T + dot_fast(middle, middle, rows_first))


def split(x):
    high = x.astype(bf16)
    return high, (x - high.astype(f32)).astype(bf16)


def tree_sum(values):
    values = list(values)
    while len(values) > 1:
        values = [a + b for a, b in zip(values[0::2], values[1::2])]
    return values[0]


def eye_mask(n):
    return lax.broadcasted_iota(jnp.int32, (n, n), 0) == lax.broadcasted_iota(jnp.int32, (n, n), 1)


def regularized(matrix):
    n = matrix.shape[0]
    eye = eye_mask(n)
    diagonal = jnp.where(eye, matrix, 0.0)
    ridge = ridge_share * jnp.sum(diagonal) / n
    return matrix + jnp.where(eye, ridge, 0.0)


def invert(matrix, x_ref, work_ref):
    n = matrix.shape[0]
    eye = eye_mask(n)
    diagonal = jnp.where(eye, matrix, 0.0)
    by_column = lax.rsqrt(jnp.sum(diagonal, axis=0, keepdims=True))
    by_row = lax.rsqrt(jnp.sum(diagonal, axis=1, keepdims=True))
    e1 = jnp.where(eye, 0.0, -(matrix * by_column) * by_row)
    e1_half = e1.astype(bf16)
    e2 = dot_fast(e1_half, e1_half)
    e2_half = e2.astype(bf16)
    e4 = dot_fast(e2_half, e2_half)
    e4_half = e4.astype(bf16)
    part = e1 + e2 + dot_fast(e1_half, e2_half)
    part = part + e4 + dot_fast(part.astype(bf16), e4_half)
    left = jnp.sum(e4 * e4)
    x_ref[...] = (part + jnp.where(eye, 1.0, 0.0)) * by_column * by_row

    @pl.when(jnp.logical_not(left < contraction_bound))
    def _():
        work_ref[...] = jnp.where(eye, 1.0, 0.0) - e1
        lane = lax.broadcasted_iota(jnp.int32, (n, n), 1)
        sublane = lax.broadcasted_iota(jnp.int32, (n, n), 0)
        lane_row = lax.broadcasted_iota(jnp.int32, (1, n), 1)

        def step(k, carry):
            work = work_ref[...]
            row = work_ref[pl.ds(k, 1), :]
            pivot = jnp.sum(jnp.where(lane_row == k, row, 0.0), axis=1, keepdims=True)
            column = jnp.sum(jnp.where(lane == k, work, 0.0), axis=1, keepdims=True)
            inverse = 1.0 / pivot
            new_row = jnp.where(lane_row == k, inverse, row * inverse)
            others = jnp.where(lane == k, 0.0, work) - column * new_row
            work_ref[...] = jnp.where(sublane == k, new_row, others)
            return carry

        lax.fori_loop(0, n, step, 0)
        x_ref[...] = work_ref[...] * by_column * by_row


def solve(right, matrix, inverse):
    first = dot(right, inverse)
    return first + dot(right - dot(first, matrix), inverse)


def place_of(axis):
    return lax.axis_index(axis)


def at_rows(block, rows):
    return pl.ds(pl.multiple_of(block * rows, rows), rows)


def load_kernel(time_hbm, species_hbm, half_ref, time_ref, species_ref, arrived):
    half = half_ref.shape[0]
    copies = [
        pltpu.make_async_copy(time_hbm.at[at_rows(place_of("space") % 2, half)], half_ref, arrived.at[0]),
        pltpu.make_async_copy(time_hbm, time_ref, arrived.at[1]),
        pltpu.make_async_copy(species_hbm, species_ref, arrived.at[2]),
    ]
    for copy in copies:
        copy.start()
    for copy in copies:
        copy.wait()


def space_kernel(tensor_ref, time_ref, species_ref, m_a_ref, side_ref):
    species = species_ref[...]
    species_count = species.shape[0]
    time_high, time_low = split(time_ref[...])
    weights = jnp.concatenate([time_high, time_low, time_low, time_high], axis=0)
    chunk = 8
    height = chunk * species_count
    for start in range(0, tensor_ref.shape[0], height):
        high, low = split(tensor_ref[start:start + height, :])
        side = dot_fast(jnp.concatenate([high, low, high, low], axis=1), weights)
        side = side.reshape(chunk, species_count, side.shape[1])
        at = start // species_count
        side_ref[at:at + chunk] = side
        m_a_ref[at:at + chunk, :] = jnp.sum(side * species[None], axis=1)


def pack_kernel(after_ref, *refs):
    *parts, out_ref = refs
    at = 0
    for part in parts:
        out_ref[at:at + part.shape[0], :] = part[...]
        at += part.shape[0]


def peers(count):
    return [(j, j + 1) for j in range(1, count - 1, 2)], count - 1


def place_blocks(factor_ref, place, core, own_ref, mine_ref, partner_ref):
    rows = own_ref.shape[0]
    half = rows // 2
    factor_ref[at_rows(place, rows), :] = own_ref[...]
    pairs, last = peers(factor_ref.shape[0] // rows)
    for i, (first, second) in enumerate(pairs):
        step = second - first
        taken = slice(i * rows, (i + 1) * rows)
        factor_ref[at_rows(jnp.bitwise_xor(place, first + core * step), rows), :] = mine_ref[taken, :]
        factor_ref[at_rows(jnp.bitwise_xor(place, second - core * step), rows), :] = partner_ref[taken, :]
    taken = slice(len(pairs) * rows, len(pairs) * rows + half)
    at = jnp.bitwise_xor(place, last) * 2
    factor_ref[at_rows(at + core, half), :] = mine_ref[taken, :]
    factor_ref[at_rows(at + 1 - core, half), :] = partner_ref[taken, :]


def sum_kernel(*refs):
    *parts, out_ref = refs
    out_ref[...] = tree_sum([part[...] for part in parts])


def time_side_kernel(species_count, first, raw_ref, tensor_ref, side_ref):
    rows = raw_ref.shape[0]
    raw_high, raw_low = split(raw_ref[...])
    weights = jnp.concatenate([raw_high, raw_high, raw_low, raw_low], axis=0)
    for p in range(side_ref.shape[0]):
        high, low = split(tensor_ref[pl.ds(first + p, rows, stride=species_count), :])
        side_ref[p] = dot_fast(jnp.concatenate([high, low, high, low], axis=0), weights, ((0,), (0,)))


def factor_gram_kernel(after_ref, species_ref, out_ref):
    out_ref[...] = gram(species_ref[...])


def first_inverse_kernel(b_gram_ref, own_ref, mine_ref, partner_ref,
                         c_gram_ref, matrix_ref, inverse_ref, factor_ref, work_ref):
    place_blocks(factor_ref, place_of("tm"), place_of("space") % 2, own_ref, mine_ref, partner_ref)
    c_gram = gram(factor_ref[...])
    c_gram_ref[...] = c_gram
    matrix = regularized(b_gram_ref[...] * c_gram)
    matrix_ref[...] = matrix
    invert(matrix, inverse_ref, work_ref)


def space_solve_kernel(matrix_ref, inverse_ref, side_ref, *refs):
    *parts, raw_ref, keep_ref, send_ref, m_b_ref = refs
    core = place_of("space") % 2
    m_a = tree_sum([part[...] for part in parts])
    raw = solve(m_a, matrix_ref[...], inverse_ref[...])
    raw_ref[...] = raw
    rows = raw.shape[0]
    send_ref[:rows, :] = raw
    total = jnp.zeros(m_b_ref.shape, f32)
    for s in range(rows):
        total = total + side_ref[s] * raw_ref[pl.ds(s, 1), :]
    m_b_ref[...] = total
    half = keep_ref.shape[0]
    keep_ref[...] = m_b_ref[at_rows(core, half), :]
    send_ref[rows:, :] = m_b_ref[at_rows(1 - core, half), :]


def chip_kernel(raw_ref, keep_ref, received_ref, block_ref, m_b_ref):
    core = place_of("space") % 2
    rows = raw_ref.shape[0]
    block_ref[at_rows(core, rows), :] = raw_ref[...]
    block_ref[at_rows(1 - core, rows), :] = received_ref[:rows, :]
    m_b_ref[...] = keep_ref[...] + received_ref[rows:, :]


def space_gram_kernel(c_gram_ref, own_ref, mine_ref, partner_ref,
                      a_gram_ref, matrix_ref, scale_ref, out_ref, factor_ref):
    place = place_of("space")
    place_blocks(factor_ref, place // 2, place % 2, own_ref, mine_ref, partner_ref)
    raw_gram = gram(factor_ref[...])
    eye = eye_mask(raw_gram.shape[0])
    diagonal = jnp.where(eye, raw_gram, 0.0)
    total_rows = factor_ref.shape[0]
    by_column = lax.rsqrt(jnp.sum(diagonal, axis=0, keepdims=True) / total_rows + epsilon)
    by_row = lax.rsqrt(jnp.sum(diagonal, axis=1, keepdims=True) / total_rows + epsilon)
    scale_ref[...] = jnp.broadcast_to(by_column, scale_ref.shape)
    out_ref[...] = own_ref[at_rows(place % 2, out_ref.shape[0]), :] * by_column
    a_gram = raw_gram * by_column * by_row
    a_gram_ref[...] = a_gram
    matrix_ref[...] = regularized(a_gram * c_gram_ref[...])


def inverse_kernel(matrix_ref, inverse_ref, work_ref):
    invert(matrix_ref[...], inverse_ref, work_ref)


def refined_inverse_kernel(matrix_ref, inverse_ref, work_ref):
    matrix = matrix_ref[...]
    invert(matrix, inverse_ref, work_ref)
    inverse = inverse_ref[...]
    left = jnp.where(eye_mask(matrix.shape[0]), 1.0, 0.0) - dot(matrix, inverse)
    inverse_ref[...] = inverse + dot(inverse, left)


def species_kernel(scale_ref, matrix_ref, inverse_ref, side_ref, rest_ref, mine_ref, partner_ref,
                   species_ref, scaled_ref, send_ref):
    core = place_of("space") % 2
    scale = scale_ref[0:1, :]
    half = mine_ref.shape[0]
    scaled_ref[at_rows(core, half), :] = mine_ref[...]
    scaled_ref[at_rows(1 - core, half), :] = partner_ref[...]
    m_b = scaled_ref[...] * scale
    raw = solve(m_b, matrix_ref[...], inverse_ref[...])
    species = raw * lax.rsqrt(jnp.mean(raw * raw, axis=0, keepdims=True) + epsilon)
    species_ref[...] = species
    scaled_ref[...] = species * scale
    time_half(1 - core, (side_ref, rest_ref), scaled_ref, send_ref)


def time_half(block, side_refs, scaled_ref, out_ref):
    half = out_ref.shape[0]
    total = jnp.zeros(out_ref.shape, f32)
    at = 0
    for side_ref in side_refs:
        for p in range(side_ref.shape[0]):
            total = total + side_ref[p, at_rows(block, half), :] * scaled_ref[at:at + 1, :]
            at += 1
    out_ref[...] = total


def time_half_kernel(side_ref, rest_ref, scaled_ref, out_ref):
    time_half(place_of("space") % 2, (side_ref, rest_ref), scaled_ref, out_ref)


def species_gram_kernel(a_gram_ref, species_ref, matrix_ref):
    matrix_ref[...] = regularized(a_gram_ref[...] * gram(species_ref[...]))


def time_solve_kernel(inverse_ref, mine_ref, partner_ref, raw_ref, squares_ref, m_c_ref):
    core = place_of("space") % 2
    half = mine_ref.shape[0]
    m_c_ref[at_rows(core, half), :] = mine_ref[...]
    m_c_ref[at_rows(1 - core, half), :] = partner_ref[...]
    raw = dot(m_c_ref[...], inverse_ref[...])
    raw_ref[...] = raw
    squares_ref[...] = jnp.broadcast_to(jnp.sum(raw * raw, axis=0, keepdims=True), squares_ref.shape)


def time_scale_kernel(total_steps, raw_ref, *refs):
    *parts, out_ref = refs
    squares = tree_sum([part[0:1, :] for part in parts])
    out_ref[...] = raw_ref[...] * lax.rsqrt(squares / total_steps + epsilon)


def exchange(value, axis, step, count):
    return lax.ppermute(value, axis, [(i, i ^ step) for i in range(count)])


def run(kernel, outs, micros, scratch=()):
    call = pl.pallas_call(
        kernel,
        out_shape=outs,
        out_specs=[vmem] * len(outs),
        scratch_shapes=list(scratch),
        cost_estimate=pl.CostEstimate(flops=int(micros * flops_per_micro), bytes_accessed=0, transcendentals=0),
        compiler_params=pltpu.CompilerParams(vmem_limit_bytes=vmem_limit),
    )

    def placed(*operands):
        return call(*[pltpu.with_memory_space_constraint(x, pltpu.VMEM) for x in operands])

    return placed


def on_device(tensor, species_factor, time_factor):
    row_count, species_count, step_count = tensor.shape
    rank = species_factor.shape[1]
    devices = lax.axis_size("space")
    blocks = lax.axis_size("tm")
    chips = devices // 2
    total_rows = row_count * devices
    total_steps = step_count * blocks

    def local(*dims):
        return pltpu.VMEM(dims, f32)

    def result(*dims):
        return jax.ShapeDtypeStruct(dims, f32)

    square = local(rank, rank)

    def over_time(value):
        return [value] + [exchange(value, "tm", j, blocks) for j in range(1, blocks)]

    def over_chips(value):
        return [value] + [exchange(value, "space", 2 * j, devices) for j in range(1, chips)]

    def to_partner(value):
        return exchange(value, "space", 1, devices)

    def block_from(block, half, axis):
        pairs, last = peers(blocks if axis == "tm" else chips)
        received = []
        for steps in pairs:
            if axis == "tm":
                turns = [
                    (s * blocks + t, s * blocks + (t ^ steps[s % 2])) for s in range(devices) for t in range(blocks)
                ]
                received.append(lax.ppermute(block, ("space", "tm"), turns))
            else:
                turns = [(s, s ^ (2 * steps[s % 2])) for s in range(devices)]
                received.append(lax.ppermute(block, "space", turns))
        step, count = (last, blocks) if axis == "tm" else (2 * last, devices)
        return received + [exchange(half, axis, step, count)]

    def pack(after, parts):
        return run(pack_kernel, [local(sum(part.shape[0] for part in parts), rank)], 0.3)(after, *parts)[0]

    def add(parts):
        return run(sum_kernel, [local(*parts[0].shape)], 0.3)(*parts)[0]

    half_steps = step_count // 2
    half_species = species_count // 2

    outside = pl.BlockSpec(memory_space=pltpu.HBM)
    time_half, time_here, species_here = pl.pallas_call(
        load_kernel,
        in_specs=[outside] * 2,
        out_specs=[vmem] * 3,
        out_shape=[local(half_steps, rank), local(step_count, rank), local(species_count, rank)],
        scratch_shapes=[pltpu.SemaphoreType.DMA((3,))],
        cost_estimate=pl.CostEstimate(flops=int(10 * flops_per_micro), bytes_accessed=10**8, transcendentals=0),
        compiler_params=pltpu.CompilerParams(vmem_limit_bytes=vmem_limit),
        name="load",
    )(*[pltpu.with_memory_space_constraint(x, pltpu.HBM) for x in (time_factor, species_factor)])
    received = block_from(time_factor, time_half, "tm")
    m_a, side = run(
        space_kernel, [local(row_count, rank), local(row_count, species_count, rank)], 2
    )(tensor.reshape(row_count * species_count, step_count), time_here, species_here)
    m_a_parts = over_time(m_a)

    mine = pack(m_a, received)
    partner = to_partner(mine)
    (b_gram,) = run(factor_gram_kernel, [square], 0.5)(mine, species_here)
    c_gram, matrix, inverse = run(
        first_inverse_kernel, [square] * 3, 2, [local(total_steps, rank), square]
    )(b_gram, time_here, mine, partner)

    raw, keep, send = run(
        space_solve_kernel,
        [local(row_count, rank), local(half_species, rank), local(row_count + half_species, rank)],
        1,
        [local(species_count, rank)],
    )(matrix, inverse, side, *m_a_parts)
    received = to_partner(send)
    early = 5 * species_count // 8
    time_sides = []
    for first, count in ((0, early), (early, species_count - early)):
        time_sides += run(
            lambda *refs, first=first: time_side_kernel(species_count, first, *refs),
            [local(count, step_count, rank)],
            2 * count / species_count,
        )(raw, tensor.reshape(row_count * species_count, step_count))
    chip_block, m_b = run(chip_kernel, [local(2 * row_count, rank), local(half_species, rank)], 0.3)(
        raw, keep, received
    )
    m_b = add(over_time(m_b))
    raw_blocks = block_from(chip_block, raw, "space")
    m_b_parts = over_chips(m_b)
    mine = pack(m_b, raw_blocks)
    partner = to_partner(mine)
    m_b = add(m_b_parts)
    m_b_partner = to_partner(m_b)
    a_gram, matrix, scale, space_out = run(
        space_gram_kernel, [square, square, local(8, rank), local(row_count, rank)], 1.5, [local(total_rows, rank)]
    )(c_gram, chip_block, mine, partner)
    (inverse,) = run(inverse_kernel, [square], 1, [square])(matrix)

    species, scaled, m_c_send = run(
        species_kernel, [local(species_count, rank), local(species_count, rank), local(half_steps, rank)], 1.5
    )(scale, matrix, inverse, *time_sides, m_b, m_b_partner)

    m_c_received = to_partner(m_c_send)
    (m_c_keep,) = run(time_half_kernel, [local(half_steps, rank)], 1)(*time_sides, scaled)
    (matrix,) = run(species_gram_kernel, [square], 0.5)(a_gram, species)
    m_c_parts = over_chips(add([m_c_keep, m_c_received]))
    (inverse,) = run(refined_inverse_kernel, [square], 1, [square])(matrix)
    m_c = add(m_c_parts)
    m_c_partner = to_partner(m_c)
    raw_time, squares = run(
        time_solve_kernel, [local(step_count, rank), local(8, rank)], 1, [local(step_count, rank)]
    )(inverse, m_c, m_c_partner)

    squares = over_time(squares)
    (time_out,) = run(
        lambda *refs: time_scale_kernel(total_steps, *refs), [result(step_count, rank)], 0.5
    )(raw_time, *squares)
    return (space_out, species, time_out)


def solution(mesh):
    placed = (P("space", None, "tm"), P(), P("tm", None))
    return jax.shard_map(
        on_device,
        mesh=mesh,
        in_specs=placed,
        out_specs=(P("space", None), P(), P("tm", None)),
        check_vma=False,
    )
```
